256 devices in a mesh: rows: 32 (over y, z), cols: 8 (over x, core).
Axes of the slice: x: 4, y: 4, z: 8, core: 2. Of those that a mesh axis runs over, the one named last changes fastest.
Arguments:
- token_ids: int32 [128, 256], P('rows'), may hold values from 0 to 8191
- keep_mask: int32 [128, 256], P('rows'), may hold values 0 or 1
- remask_order: int32 [32768], P('rows'), may hold values from 0 to 32767, each once
- embed_table: bfloat16 [8192, 1024], P(None, 'cols'), may hold values from -6 to 6
- mask_embed: bfloat16 [1024], P('cols'), may hold values from -4 to 4
- conv_one: bfloat16 [3, 3, 1024, 1024], P(None, None, None, 'cols'), may hold values from -0.0625 to 0.0625
- gain_one: float32 [1024], P('cols'), may hold values from 0.25 to 1.75
- bias_one: float32 [1024], P('cols'), may hold values from -3 to 3
- conv_two: bfloat16 [3, 3, 1024, 1024], P(None, None, None, 'cols'), may hold values from -0.0625 to 0.0625
- gain_two: float32 [1024], P('cols'), may hold values from 0.25 to 1.75
- bias_two: float32 [1024], P('cols'), may hold values from -3 to 3
- head_weight: bfloat16 [1024, 8192], P(None, 'cols'), may hold values from -15.6 to 15.6
Outputs:
- features: bfloat16 [128, 256, 1024], P('rows', None, 'cols')
- token_logp: float32 [128, 256], P('rows', 'cols')
The draws below stay inside these ranges and needn't reach their ends.
Inputs may be any that keep to these rules, and one draw needn't show every extreme that they name: `remask_order`: each rank appears once.
All inputs are finite; a program needn't handle non-finite values. No bound on the sum of `keep_mask` on one device may be relied on, other than what follows from the above.
Results may differ from the reference program's by a relative error of at most 0.0039.
Values may be sent and summed in bfloat16 or wider, within the bound.
A program may use at most 128 MiB of HBM per device.

```python
import math
import jax
import jax.numpy as jnp
import numpy as np
from jax import lax

C = 1024
V = 8192
GROUPS = 32
W = 256
H = 128
REMASK = 16384


def draw_head_weight(key, part):
    base_key, shared_key = jax.random.split(jax.random.fold_in(key, 7))
    base = 0.1 * jnp.clip(jax.random.normal(base_key, (C, V), jnp.float32), -6.0, 6.0)
    shared = jnp.clip(jax.random.normal(shared_key, (C, 1), jnp.float32), -4.0, 4.0) * (120.0 / math.sqrt(C))
    return (base + shared).astype(jnp.bfloat16)


def plant(entries, key, least, high):
    index_at = [jax.random.randint(jax.random.fold_in(key, axis), (), 0, length) for axis, length in enumerate(entries.shape)]
    widest = entries.shape.index(max(entries.shape))
    next_to = index_at[:widest] + [(index_at[widest] + 1) % entries.shape[widest]] + index_at[widest + 1:]
    return entries.at[tuple(index_at)].set(least).at[tuple(next_to)].set(high)


def block_levels(key, dims, cuts, smallest, high):
    loudness, own = 1.0, jax.random.fold_in(key, 6)
    for axis_at, blocks in cuts:
        heights = jnp.exp(jax.random.uniform(jax.random.fold_in(own, axis_at), (blocks,), jnp.float32, smallest / len(cuts), high / len(cuts)))
        loudness = loudness * jnp.repeat(heights, dims[axis_at] // blocks).reshape([-1 if axis == axis_at else 1 for axis in range(len(dims))])
    return loudness


def rank_table(number_of, lean):
    loads = [(1 << 20) // math.isqrt(standing ** lean) + 1 for standing in range(1, number_of + 1)]
    scale = 1 + sum(loads) // (1 << 30)
    return np.cumsum(np.array([max(1, weight // scale) for weight in loads]))


def ranked_ids(stream_key, extent, count, slope):
    grid = rank_table(count, slope)
    pick = jax.random.randint(jax.random.fold_in(stream_key, 1), extent, 0, int(grid[count - 1]))
    standing = jnp.searchsorted(jnp.asarray(grid, jnp.int32), pick, side="right")
    return jax.random.permutation(jax.random.fold_in(stream_key, 2), count)[standing].astype(jnp.int32)


def centred(own_key, extent, scale, reach, cuts=(), dtype=jnp.bfloat16):
    level = block_levels(own_key, extent, cuts, -0.22, 0.18) if cuts else 1.0
    array = jax.random.normal(own_key, extent, jnp.float32) * scale * level
    return jnp.minimum(jnp.maximum(array, -reach), reach).astype(dtype)


def setup_inputs(seed: int = 0) -> dict:
    key_of = jax.random.split(jax.random.key(seed), 13)
    return {
        "token_ids": plant(ranked_ids(key_of[0], (H, W), V, 2), jax.random.fold_in(key_of[0], 3), 0, V - 1).astype(jnp.int32),
        "keep_mask": plant((jax.random.randint(key_of[1], (H, W), 0, 4) < 1).astype(jnp.int32), jax.random.fold_in(key_of[1], 1), 0, 1),
        "remask_order": jax.random.permutation(key_of[2], H * W).astype(jnp.int32),
        "embed_table": centred(key_of[3], (V, C), 1.0, 6.0, ((1, 8),)),
        "mask_embed": centred(key_of[4], (C,), 1.0, 4.0, ((0, 8),)),
        "conv_one": centred(key_of[5], (3, 3, C, C), (9 * C) ** -0.5, 0.0625, ((3, 8),)),
        "gain_one": jnp.clip(1.0 + 0.15 * jax.random.normal(key_of[6], (C,), jnp.float32), 0.25, 1.75),
        "bias_one": centred(key_of[7], (C,), 0.5, 3.0, ((0, 8),), jnp.float32),
        "conv_two": centred(key_of[8], (3, 3, C, C), (9 * C) ** -0.5, 0.0625, ((3, 8),)),
        "gain_two": jnp.clip(1.0 + 0.15 * jax.random.normal(key_of[9], (C,), jnp.float32), 0.25, 1.75),
        "bias_two": centred(key_of[10], (C,), 0.5, 3.0, ((0, 8),), jnp.float32),
        "head_weight": draw_head_weight(jax.random.fold_in(key_of[12], 71), 0),
    }


def convolve(field, weight):
    height, width, channels = field.shape
    padded = jnp.pad(field, ((1, 1), (1, 1), (0, 0)))
    total = jnp.zeros((height * width, weight.shape[3]), jnp.float32)
    for shift_row in range(3):
        for shift_col in range(3):
            window = padded[shift_row:shift_row + height, shift_col:shift_col + width].reshape(-1, channels)
            total = total + jnp.dot(window, weight[shift_row, shift_col], preferred_element_type=jnp.float32)
    return total.reshape(height, width, -1)

def group_norm(values, gain, bias):
    height, width, channels = values.shape
    flat = values.reshape(height * width, GROUPS, channels // GROUPS)
    mean = lax.optimization_barrier(jnp.mean(flat, axis=(0, 2)))
    deviation = flat - mean[None, :, None]
    variance = lax.optimization_barrier(jnp.mean(deviation * deviation, axis=(0, 2)))
    normed = deviation / jnp.sqrt(variance + 1e-05)[None, :, None]
    return normed.reshape(height, width, channels) * gain + bias

def reference(token_ids, keep_mask, remask_order, embed_table, mask_embed, conv_one, gain_one, bias_one, conv_two, gain_two, bias_two, head_weight):
    order = remask_order.reshape(token_ids.shape)
    visible = (keep_mask == 1) | (order >= REMASK)
    looked = jnp.take(embed_table, token_ids, axis=0)
    start = jnp.where(visible[:, :, None], looked, mask_embed[None, None, :])
    hidden = jax.nn.silu(group_norm(convolve(start, conv_one), gain_one, bias_one)).astype(jnp.bfloat16)
    second = group_norm(convolve(hidden, conv_two), gain_two, bias_two)
    features = (start.astype(jnp.float32) + second).astype(jnp.bfloat16)

    def row_logp(inputs):
        feature_row, id_row = inputs
        logits = jnp.dot(feature_row, head_weight, preferred_element_type=jnp.float32)
        top = lax.optimization_barrier(jnp.max(logits, axis=1))
        total = jnp.log(lax.optimization_barrier(jnp.sum(jnp.exp(logits - top[:, None]), axis=1))) + top
        picked = jnp.take_along_axis(logits, id_row[:, None].astype(jnp.int32), axis=1)[:, 0]
        return picked - total
    token_logp = lax.map(row_logp, (features, token_ids))
    return (features, token_logp)
```

```python
import functools

import jax
import jax.numpy as jnp
from jax import lax
from jax.experimental import pallas as pl
from jax.experimental.pallas import tpu as pltpu
from jax.sharding import PartitionSpec as P

GROUP_WIDTH = 32
MESH = pl.DeviceIdType.MESH
F32 = jnp.float32
BF16 = jnp.bfloat16
XP, XM, OWN, FROM_P, FROM_M, FAR, FWD, UP, DOWN, UPF, DOWNF = range(11)


def group_sum(row):
    width = row.shape[1]
    a = lax.broadcasted_iota(jnp.int32, (width, width), 0) // GROUP_WIDTH
    b = lax.broadcasted_iota(jnp.int32, (width, width), 1) // GROUP_WIDTH
    ones = jnp.where(a == b, 1.0, 0.0).astype(F32)
    rows = jnp.broadcast_to(row, (8, width))
    return jnp.dot(
        rows, ones, preferred_element_type=F32, precision=lax.Precision.HIGHEST
    )[0:1]


def kernel(
    num_rows,
    num_cols,
    ids_ref,
    keep_ref,
    order_ref,
    table_hbm,
    mask_ref,
    conv_one_hbm,
    gain_one_ref,
    bias_one_ref,
    conv_two_hbm,
    gain_two_ref,
    bias_two_ref,
    head_hbm,
    features_ref,
    logp_ref,
    table_ref,
    wide_ref,
    conv_one_ref,
    conv_two_ref,
    head_ref,
    ids_vmem,
    ids_smem,
    tokens_ref,
    looked_ref,
    field_one,
    field_two,
    field_three,
    total_ref,
    conv_ref,
    stat_send,
    stat_all,
    logits_ref,
    last_send,
    last_all,
    load_sems,
    send_sems,
    recv_sems,
    stat_send_sems,
    stat_recv_sems,
    last_send_sems,
    last_recv_sems,
):
    height, width = ids_ref.shape
    vocab = table_hbm.shape[0]
    lanes = table_hbm.shape[1]
    channels = num_cols * lanes
    r = lax.axis_index("rows")
    k = lax.axis_index("cols")
    chips = num_cols // 2
    core = lax.rem(k, 2)
    chip = k // 2
    partner = k + 1 - 2 * core

    def piece(step, c):
        return lax.rem(chip + step, chips) * 2 + c

    right, left = piece(1, core), piece(chips - 1, core)
    above = lax.rem(r + num_rows - 1, num_rows)
    below = lax.rem(r + 1, num_rows)

    loads = [
        pltpu.make_async_copy(src, dst, load_sems.at[n])
        for n, (src, dst) in enumerate(
            (
                (table_hbm, table_ref),
                (conv_one_hbm, conv_one_ref),
                (conv_two_hbm, conv_two_ref),
                (head_hbm, head_ref),
            )
        )
    ]
    for load in loads:
        load.start()

    barrier = pltpu.get_barrier_semaphore()

    def greet_row(d, _):
        pl.semaphore_signal(
            barrier,
            inc=1,
            device_id={"rows": lax.rem(r + d, num_rows)},
            device_id_type=MESH,
        )
        return 0

    def greet_col(d, _):
        pl.semaphore_signal(
            barrier,
            inc=1,
            device_id={"cols": lax.rem(k + d, num_cols)},
            device_id_type=MESH,
        )
        return 0

    lax.fori_loop(1, num_rows, greet_row, 0)
    lax.fori_loop(1, num_cols, greet_col, 0)

    half = height * width * num_rows // 2
    parts = width // 128
    for i in range(height):
        for j in range(parts):
            at = (slice(i, i + 1), slice(128 * j, 128 * j + 128))
            n = i * parts + j
            visible = (keep_ref[at] == 1) | (order_ref[n : n + 1, :] >= half)
            ids_vmem[n : n + 1, :] = jnp.where(visible, ids_ref[at], vocab)
    to_smem = pltpu.make_async_copy(ids_vmem, ids_smem, load_sems.at[4])
    to_smem.start()
    for i in range(height):
        row = ids_ref[i : i + 1, :].astype(F32)
        tokens_ref[i] = jnp.broadcast_to(row, (128, width)).T
    loads[0].wait()
    step_rows = 512

    def widen(n, _):
        at = pl.ds(pl.multiple_of(n * step_rows, step_rows), step_rows)
        wide_ref[at, :] = table_ref[at, :].astype(F32)
        return 0

    lax.fori_loop(0, vocab // step_rows, widen, 0)
    wide_ref[vocab : vocab + 8, :] = jnp.broadcast_to(mask_ref[...].astype(F32), (8, lanes))
    to_smem.wait()

    pl.semaphore_wait(barrier, num_rows - 1 + num_cols - 1)

    pending = []

    class Gather:
        def __init__(self, n, field, halo):
            self.n, self.field, self.halo = n, field, halo
            self.off = 1 if halo else 0

        def copy(self, kind, slot, owner, row, device, to_row=None):
            to_row = row if to_row is None else to_row
            return pltpu.make_async_remote_copy(
                src_ref=self.field.at[owner, row],
                dst_ref=self.field.at[owner, to_row],
                send_sem=send_sems.at[self.n, kind, slot],
                recv_sem=recv_sems.at[self.n, kind, slot],
                device_id=device,
                device_id_type=MESH,
            )

        def send(self, *args, **kw):
            c = self.copy(*args, **kw)
            c.start()
            pending.append(c)

        def wait(self, kind, slot, owner, row):
            self.copy(kind, slot, owner, row, {"cols": partner}).wait_recv()

        def halo_out(self, q, owner, i):
            if not self.halo:
                return
            if i == 0:
                self.send(UP, q, owner, 1, {"rows": above}, to_row=height + 1)
            if i == height - 1:
                self.send(DOWN, q, owner, height, {"rows": below}, to_row=0)

        def own(self, i):
            row = i + self.off
            self.send(XP, i, k, row, {"cols": right})
            self.send(XM, i, k, row, {"cols": left})
            self.halo_out(0, k, i)
            self.send(OWN, i, k, row, {"cols": partner})

        def from_left(self, i):
            row, owner = i + self.off, left
            self.wait(XP, i, owner, row)
            if i in (0, 1):
                self.send(FWD, i, owner, row, {"cols": right})
            self.halo_out(1, owner, i)
            self.send(FROM_P, i, owner, row, {"cols": partner})

        def from_right(self, i):
            row, owner = i + self.off, right
            self.wait(XM, i, owner, row)
            if i in (2, 3):
                self.send(FWD, i, owner, row, {"cols": left})
            self.halo_out(2, owner, i)
            self.send(FROM_M, i, owner, row, {"cols": partner})

        def from_far(self, i):
            row, owner = i + self.off, piece(2, core)
            self.wait(FWD, i, owner, row)
            self.halo_out(3, owner, i)
            self.send(FAR, i, owner, row, {"cols": partner})

        def owner_of(self, q, c):
            return piece((0, chips - 1, 1, 2)[q], c)

        def halo_in(self, q):
            owner = self.owner_of(q, core)
            self.wait(UP, q, owner, height + 1)
            self.send(UPF, q, owner, height + 1, {"cols": partner})
            self.wait(DOWN, q, owner, 0)
            self.send(DOWNF, q, owner, 0, {"cols": partner})

        def rest(self, q):
            owner = self.owner_of(q, 1 - core)
            for i in range(height):
                self.wait((OWN, FROM_P, FROM_M, FAR)[q], i, owner, i + self.off)
            if self.halo:
                self.wait(UPF, q, owner, height + 1)
                self.wait(DOWNF, q, owner, 0)

    def convolve(gather, weight_ref, q):
        field = gather.field
        at = lax.rem(chip + (0, chips - 1, 1, 2)[q], chips)
        one, two = at * 2, at * 2 + 1
        rows = pl.ds(pl.multiple_of(at * 2 * lanes, 2 * lanes), 2 * lanes)
        weights = jnp.concatenate(
            [
                jnp.concatenate([weight_ref[a, b, rows, :] for b in range(3)], axis=1)
                for a in range(3)
            ],
            axis=0,
        )
        tall = 2

        def block(n, _):
            first = n * tall
            keep_up = jnp.logical_or(r > 0, n > 0)
            keep_down = jnp.logical_or(r < num_rows - 1, n < height // tall - 1)
            columns = []
            for a in range(3):
                for p in (one, two):
                    tiles = [field[p, first + a + t] for t in range(tall)]
                    if a == 0:
                        tiles[0] = jnp.where(keep_up, tiles[0], jnp.zeros_like(tiles[0]))
                    if a == 2:
                        tiles[-1] = jnp.where(keep_down, tiles[-1], jnp.zeros_like(tiles[-1]))
                    columns.append(jnp.concatenate(tiles, axis=0))
            product = jnp.dot(
                jnp.concatenate(columns, axis=1), weights, preferred_element_type=F32
            )
            at_rows = pl.ds(pl.multiple_of(first * width, tall * width), tall * width)
            if q == 0:
                total_ref[at_rows, :] = product
            else:
                total_ref[at_rows, :] += product
            return 0

        lax.fori_loop(0, height // tall, block, 0)

    def shifted_sum():
        index = lax.broadcasted_iota(jnp.int32, (width, lanes), 0)
        for i in range(height):
            at = slice(i * width, (i + 1) * width)
            before = pltpu.roll(total_ref[at, 0:lanes], 1, axis=0)
            after = pltpu.roll(total_ref[at, 2 * lanes : 3 * lanes], width - 1, axis=0)
            conv_ref[at, :] = (
                jnp.where(index == 0, 0.0, before)
                + total_ref[at, lanes : 2 * lanes]
                + jnp.where(index == width - 1, 0.0, after)
            )

    def statistics(n):
        count = height * width * GROUP_WIDTH
        values = conv_ref[...]
        mean = group_sum(jnp.sum(values, axis=0, keepdims=True)) / count
        deviation = values - mean
        square = group_sum(jnp.sum(deviation * deviation, axis=0, keepdims=True))
        both = jnp.concatenate([mean, square], axis=0)
        stat_send[n] = both

        def tell(d, _):
            to = lax.rem(r + d, num_rows)
            pltpu.make_async_remote_copy(
                src_ref=stat_send.at[n],
                dst_ref=stat_all.at[n, d],
                send_sem=stat_send_sems.at[n],
                recv_sem=stat_recv_sems.at[n],
                device_id={"rows": to},
                device_id_type=MESH,
            ).start()
            return 0

        lax.fori_loop(1, num_rows, tell, 0)
        stat_all[n, 0] = both
        everything = stat_all.at[n, pl.ds(1, num_rows - 1)]
        arrived = pltpu.make_async_remote_copy(
            src_ref=everything,
            dst_ref=everything,
            send_sem=stat_send_sems.at[n],
            recv_sem=stat_recv_sems.at[n],
            device_id={"rows": above},
            device_id_type=MESH,
        )
        arrived.wait_recv()
        pending.append(arrived)
        stats = stat_all[n]
        means = stats[:, 0, :]
        mean = jnp.sum(means, axis=0, keepdims=True) / num_rows
        spread = means - mean
        square = jnp.sum(stats[:, 1, :], axis=0, keepdims=True)
        square = square + count * jnp.sum(spread * spread, axis=0, keepdims=True)
        return mean, square / (count * num_rows)

    first = Gather(0, field_one, True)

    def look_up(i):
        unroll = 16

        def some(n, _):
            base = n * unroll
            line = i * parts + base // 128
            lane = lax.rem(base, 128)
            for u in range(unroll):
                row = ids_smem[line, lane + u]
                looked_ref[pl.ds(base + u, 1), :] = wide_ref[pl.ds(row, 1), :]
            return 0

        lax.fori_loop(0, width // unroll, some, 0)
        first.field[k, i + 1] = looked_ref[...].astype(BF16)

    def run_gather(gather, make, early):
        make(0)
        gather.own(0)
        make(3)
        gather.own(3)
        make(1)
        gather.own(1)
        gather.from_left(0)
        gather.from_right(3)
        make(2)
        gather.own(2)
        gather.from_right(0)
        gather.from_left(3)
        if gather.halo:
            gather.halo_in(0)
        gather.rest(0)
        early()
        gather.from_left(1)
        gather.from_right(2)
        if gather.halo:
            gather.halo_in(1)
            gather.halo_in(2)
        gather.from_right(1)
        gather.from_left(2)
        gather.from_far(0)
        gather.from_far(3)

    def conv_layer(gather, make, load, weight_ref, n):
        def early():
            load.wait()
            convolve(gather, weight_ref, 0)

        run_gather(gather, make, early)
        gather.rest(1)
        convolve(gather, weight_ref, 1)
        gather.from_far(1)
        gather.from_far(2)
        gather.halo_in(3)
        gather.rest(2)
        convolve(gather, weight_ref, 2)
        gather.rest(3)
        convolve(gather, weight_ref, 3)
        shifted_sum()
        return statistics(n)

    mean, variance = conv_layer(first, look_up, loads[1], conv_one_ref, 0)

    second = Gather(1, field_two, True)
    root_one = jnp.sqrt(variance + 1e-5)
    gain_one = gain_one_ref[...]
    bias_one = bias_one_ref[...]

    def make_hidden(i):
        at = slice(i * width, (i + 1) * width)
        v = (conv_ref[at, :] - mean) / root_one * gain_one + bias_one
        second.field[k, i + 1] = (v / (1.0 + jnp.exp(-v))).astype(BF16)

    mean_two, variance_two = conv_layer(second, make_hidden, loads[2], conv_two_ref, 1)

    third = Gather(2, field_three, False)
    root_two = jnp.sqrt(variance_two + 1e-5)
    gain_two = gain_two_ref[...]
    bias_two = bias_two_ref[...]

    def make_features(i):
        at = slice(i * width, (i + 1) * width)
        v = (conv_ref[at, :] - mean_two) / root_two * gain_two + bias_two
        out = (first.field[k, i + 1].astype(F32) + v).astype(BF16)
        third.field[k, i] = out
        features_ref[i] = out

    vocab_here = head_hbm.shape[1]
    tiles = vocab_here // 128

    def head_row(i):
        left_side = jnp.concatenate([third.field[p, i] for p in range(num_cols)], axis=1)
        logits_ref[...] = jnp.dot(left_side, head_ref[...], preferred_element_type=F32)
        most = logits_ref[:, 0:128]
        for t in range(1, tiles):
            most = jnp.maximum(most, logits_ref[:, 128 * t : 128 * t + 128])
        top = jnp.max(most, axis=1, keepdims=True)
        token = tokens_ref[i]
        lane = lax.broadcasted_iota(jnp.int32, (width, 128), 1)
        summed = jnp.zeros((width, 128), F32)
        picked = jnp.zeros((width, 128), F32)
        for t in range(tiles):
            part = logits_ref[:, 128 * t : 128 * t + 128]
            summed = summed + jnp.exp(part - top)
            ids = (lane + (k * vocab_here + 128 * t)).astype(F32)
            picked = picked + jnp.where(ids == token, part, 0.0)
        top_row = jnp.max(most.T, axis=0, keepdims=True)
        sum_row = jnp.sum(summed.T, axis=0, keepdims=True)
        pick_row = jnp.sum(picked.T, axis=0, keepdims=True)
        for s, row in enumerate((top_row, sum_row, pick_row)):
            for b in range(parts):
                last_send[b, s, pl.ds(i, 1), :] = row[:, 128 * b : 128 * b + 128]

    def head_rows(start, step):
        def one(n, _):
            head_row(start + step * n)
            return 0

        lax.fori_loop(0, 2, one, 0)

    run_gather(third, make_features, lambda: None)
    for q in range(1, 4):
        for i in (0, 3):
            third.wait((OWN, FROM_P, FROM_M, FAR)[q], i, third.owner_of(q, 1 - core), i)
    loads[3].wait()
    head_rows(0, 3)
    third.from_far(1)
    third.from_far(2)
    for q in range(1, 4):
        for i in (1, 2):
            third.wait((OWN, FROM_P, FROM_M, FAR)[q], i, third.owner_of(q, 1 - core), i)
    head_rows(1, 1)

    per_block = num_cols // parts

    def exchange(d):
        to = lax.rem(k + d, num_cols)
        return pltpu.make_async_remote_copy(
            src_ref=last_send.at[to // per_block],
            dst_ref=last_all.at[d],
            send_sem=last_send_sems.at[d],
            recv_sem=last_recv_sems.at[d],
            device_id={"cols": to},
            device_id_type=MESH,
        )

    for d in range(1, num_cols):
        exchange(d).start()
    last_all[0] = last_send[k // per_block]
    for d in range(1, num_cols):
        exchange(d).wait_recv()
    top = last_all[0, 0]
    for d in range(1, num_cols):
        top = jnp.maximum(top, last_all[d, 0])
    summed = jnp.zeros_like(top)
    picked = jnp.zeros_like(top)
    for d in range(num_cols):
        summed = summed + last_all[d, 1] * jnp.exp(last_all[d, 0] - top)
        picked = picked + last_all[d, 2]
    logp = picked - top - jnp.log(summed)
    mine = width // num_cols
    place = lax.rem(k, per_block)
    out = logp[:, 0:mine]
    for b in range(1, per_block):
        out = jnp.where(place == b, logp[:, mine * b : mine * b + mine], out)
    logp_ref[...] = out

    for copy in pending:
        copy.wait_send()
    for d in range(1, num_cols):
        exchange(d).wait_send()


def local(
    token_ids,
    keep_mask,
    remask_order,
    embed_table,
    mask_embed,
    conv_one,
    gain_one,
    bias_one,
    conv_two,
    gain_two,
    bias_two,
    head_weight,
):
    num_rows, num_cols = lax.axis_size("rows"), lax.axis_size("cols")
    height, width = token_ids.shape
    vocab, lanes = embed_table.shape
    lines = height * width // 128
    in_vmem = pl.BlockSpec(memory_space=pltpu.VMEM)
    anywhere = pl.BlockSpec(memory_space=pl.ANY)
    return pl.pallas_call(
        functools.partial(kernel, num_rows, num_cols),
        name="denoise",
        out_shape=(
            jax.ShapeDtypeStruct((height, width, lanes), BF16),
            jax.ShapeDtypeStruct((height, width // num_cols), F32),
        ),
        in_specs=[
            in_vmem,
            in_vmem,
            in_vmem,
            anywhere,
            in_vmem,
            anywhere,
            in_vmem,
            in_vmem,
            anywhere,
            in_vmem,
            in_vmem,
            anywhere,
        ],
        out_specs=(in_vmem, in_vmem),
        scratch_shapes=[
            pltpu.VMEM((vocab, lanes), BF16),
            pltpu.VMEM((vocab + 8, lanes), F32),
            pltpu.VMEM(conv_one.shape, BF16),
            pltpu.VMEM(conv_two.shape, BF16),
            pltpu.VMEM(head_weight.shape, BF16),
            pltpu.VMEM((lines, 128), jnp.int32),
            pltpu.SMEM((lines, 128), jnp.int32),
            pltpu.VMEM((height, width, 128), F32),
            pltpu.VMEM((width, lanes), F32),
            pltpu.VMEM((num_cols, height + 2, width, lanes), BF16),
            pltpu.VMEM((num_cols, height + 2, width, lanes), BF16),
            pltpu.VMEM((num_cols, height, width, lanes), BF16),
            pltpu.VMEM((height * width, 3 * lanes), F32),
            pltpu.VMEM((height * width, lanes), F32),
            pltpu.VMEM((2, 2, lanes), F32),
            pltpu.VMEM((2, num_rows, 2, lanes), F32),
            pltpu.VMEM((width, head_weight.shape[1]), F32),
            pltpu.VMEM((width // 128, 3, height, 128), F32),
            pltpu.VMEM((num_cols, 3, height, 128), F32),
            pltpu.SemaphoreType.DMA((5,)),
            pltpu.SemaphoreType.DMA((3, 11, 4)),
            pltpu.SemaphoreType.DMA((3, 11, 4)),
            pltpu.SemaphoreType.DMA((2,)),
            pltpu.SemaphoreType.DMA((2,)),
            pltpu.SemaphoreType.DMA((num_cols,)),
            pltpu.SemaphoreType.DMA((num_cols,)),
        ],
        compiler_params=pltpu.CompilerParams(
            collective_id=0, has_side_effects=True, vmem_limit_bytes=60 * 1024 * 1024
        ),
    )(
        token_ids,
        keep_mask,
        remask_order.reshape(lines, 128),
        embed_table,
        mask_embed.reshape(1, lanes),
        conv_one,
        gain_one.reshape(1, lanes),
        bias_one.reshape(1, lanes),
        conv_two,
        gain_two.reshape(1, lanes),
        bias_two.reshape(1, lanes),
        head_weight,
    )


def solution(mesh):
    in_specs = (
        P("rows", None),
        P("rows", None),
        P("rows"),
        P(None, "cols"),
        P("cols"),
        P(None, None, None, "cols"),
        P("cols"),
        P("cols"),
        P(None, None, None, "cols"),
        P("cols"),
        P("cols"),
        P(None, "cols"),
    )
    out_specs = (P("rows", None, "cols"), P("rows", "cols"))
    return jax.shard_map(local, mesh=mesh, in_specs=in_specs, out_specs=out_specs, check_vma=False)
```

```python
import functools

import jax
import jax.numpy as jnp
from jax import lax
from jax.experimental import pallas as pl
from jax.experimental.pallas import tpu as pltpu
from jax.sharding import PartitionSpec as P

GROUP_WIDTH = 32
MESH = pl.DeviceIdType.MESH
F32 = jnp.float32
BF16 = jnp.bfloat16
XP, XM, OWN, FROM_P, FROM_M, FAR, FWD, UP, DOWN, UPF, DOWNF = range(11)


def group_sum(row):
    width = row.shape[1]
    a = lax.broadcasted_iota(jnp.int32, (width, width), 0) // GROUP_WIDTH
    b = lax.broadcasted_iota(jnp.int32, (width, width), 1) // GROUP_WIDTH
    ones = jnp.where(a == b, 1.0, 0.0).astype(F32)
    rows = jnp.broadcast_to(row, (8, width))
    return jnp.dot(
        rows, ones, preferred_element_type=F32, precision=lax.Precision.HIGHEST
    )[0:1]


def kernel(
    num_rows,
    num_cols,
    ids_ref,
    keep_ref,
    order_ref,
    table_hbm,
    mask_ref,
    conv_one_hbm,
    gain_one_ref,
    bias_one_ref,
    conv_two_hbm,
    gain_two_ref,
    bias_two_ref,
    head_hbm,
    features_ref,
    logp_ref,
    table_ref,
    wide_ref,
    conv_one_ref,
    conv_two_ref,
    head_ref,
    ids_vmem,
    ids_smem,
    tokens_ref,
    looked_ref,
    field_one,
    field_two,
    field_three,
    total_ref,
    conv_ref,
    stat_send,
    stat_all,
    coef_send,
    coef_all,
    hidden_ref,
    logits_ref,
    last_send,
    last_all,
    load_sems,
    send_sems,
    recv_sems,
    stat_send_sems,
    stat_recv_sems,
    coef_send_sems,
    coef_recv_sems,
    last_send_sems,
    last_recv_sems,
):
    height, width = ids_ref.shape
    vocab = table_hbm.shape[0]
    lanes = table_hbm.shape[1]
    channels = num_cols * lanes
    r = lax.axis_index("rows")
    k = lax.axis_index("cols")
    chips = num_cols // 2
    core = lax.rem(k, 2)
    chip = k // 2
    partner = k + 1 - 2 * core

    def piece(step, c):
        return lax.rem(chip + step, chips) * 2 + c

    right, left = piece(1, core), piece(chips - 1, core)
    above = lax.rem(r + num_rows - 1, num_rows)
    below = lax.rem(r + 1, num_rows)

    loads = [
        pltpu.make_async_copy(src, dst, load_sems.at[n])
        for n, (src, dst) in enumerate(
            (
                (table_hbm, table_ref),
                (conv_one_hbm, conv_one_ref),
                (conv_two_hbm, conv_two_ref),
                (head_hbm, head_ref),
            )
        )
    ]
    for load in loads:
        load.start()

    barrier = pltpu.get_barrier_semaphore()

    def greet_row(d, _):
        pl.semaphore_signal(
            barrier,
            inc=1,
            device_id={"rows": lax.rem(r + d, num_rows)},
            device_id_type=MESH,
        )
        return 0

    def greet_col(d, _):
        pl.semaphore_signal(
            barrier,
            inc=1,
            device_id={"cols": lax.rem(k + d, num_cols)},
            device_id_type=MESH,
        )
        return 0

    lax.fori_loop(1, num_rows, greet_row, 0)
    lax.fori_loop(1, num_cols, greet_col, 0)

    half = height * width * num_rows // 2
    parts = width // 128
    for i in range(height):
        for j in range(parts):
            at = (slice(i, i + 1), slice(128 * j, 128 * j + 128))
            n = i * parts + j
            visible = (keep_ref[at] == 1) | (order_ref[n : n + 1, :] >= half)
            ids_vmem[n : n + 1, :] = jnp.where(visible, ids_ref[at], vocab)
    to_smem = pltpu.make_async_copy(ids_vmem, ids_smem, load_sems.at[4])
    to_smem.start()
    for i in range(height):
        row = ids_ref[i : i + 1, :].astype(F32)
        tokens_ref[i] = jnp.broadcast_to(row, (128, width)).T
    loads[0].wait()
    step_rows = 512

    def widen(n, _):
        at = pl.ds(pl.multiple_of(n * step_rows, step_rows), step_rows)
        wide_ref[at, :] = table_ref[at, :].astype(F32)
        return 0

    lax.fori_loop(0, vocab // step_rows, widen, 0)
    wide_ref[vocab : vocab + 8, :] = jnp.broadcast_to(mask_ref[...].astype(F32), (8, lanes))
    to_smem.wait()

    pending = []

    class Gather:
        def __init__(self, n, field, halo):
            self.n, self.field, self.halo = n, field, halo
            self.off = 1 if halo else 0

        def copy(self, kind, slot, owner, row, device, to_row=None):
            to_row = row if to_row is None else to_row
            return pltpu.make_async_remote_copy(
                src_ref=self.field.at[owner, row],
                dst_ref=self.field.at[owner, to_row],
                send_sem=send_sems.at[self.n, kind, slot],
                recv_sem=recv_sems.at[self.n, kind, slot],
                device_id=device,
                device_id_type=MESH,
            )

        def send(self, *args, **kw):
            c = self.copy(*args, **kw)
            c.start()
            pending.append(c)

        def wait(self, kind, slot, owner, row):
            self.copy(kind, slot, owner, row, {"cols": partner}).wait_recv()

        def halo_out(self, q, owner, i):
            if not self.halo:
                return
            if i == 0:
                self.send(UP, q, owner, 1, {"rows": above}, to_row=height + 1)
            if i == height - 1:
                self.send(DOWN, q, owner, height, {"rows": below}, to_row=0)

        def own(self, i):
            row = i + self.off
            self.halo_out(0, k, i)
            self.send(OWN, i, k, row, {"cols": partner})

        def own_right(self, i):
            self.send(XP, i, k, i + self.off, {"cols": right})

        def own_left(self, i):
            self.send(XM, i, k, i + self.off, {"cols": left})

        def from_left(self, i):
            row, owner = i + self.off, left
            self.wait(XP, i, owner, row)
            if i in (0, 1):
                self.send(FWD, i, owner, row, {"cols": right})
            self.halo_out(1, owner, i)
            self.send(FROM_P, i, owner, row, {"cols": partner})

        def from_right(self, i):
            row, owner = i + self.off, right
            self.wait(XM, i, owner, row)
            if i in (2, 3):
                self.send(FWD, i, owner, row, {"cols": left})
            self.halo_out(2, owner, i)
            self.send(FROM_M, i, owner, row, {"cols": partner})

        def from_far(self, i):
            row, owner = i + self.off, piece(2, core)
            self.wait(FWD, i, owner, row)
            self.halo_out(3, owner, i)
            self.send(FAR, i, owner, row, {"cols": partner})

        def owner_of(self, q, c):
            return piece((0, chips - 1, 1, 2)[q], c)

        def halo_in(self, q):
            owner = self.owner_of(q, core)
            self.wait(UP, q, owner, height + 1)
            self.send(UPF, q, owner, height + 1, {"cols": partner})
            self.wait(DOWN, q, owner, 0)
            self.send(DOWNF, q, owner, 0, {"cols": partner})

        def rest(self, q):
            owner = self.owner_of(q, 1 - core)
            for i in range(height):
                self.wait((OWN, FROM_P, FROM_M, FAR)[q], i, owner, i + self.off)
            if self.halo:
                self.wait(UPF, q, owner, height + 1)
                self.wait(DOWNF, q, owner, 0)

    def at_chip(q):
        return lax.rem(chip + (0, chips - 1, 1, 2)[q], chips)

    def normalise(gather, q, slots):
        for c in range(2):
            owner = at_chip(q) * 2 + c
            d = lax.rem(k - owner + num_cols, num_cols)
            scale = coef_all[0, d, 0:1, :]
            for slot in slots:
                which = 1 + jnp.where(slot > 0, 1, 0) + jnp.where(slot > height, 1, 0)
                shift = coef_all[0, d, pl.ds(which, 1), :]
                inside = jnp.logical_and(
                    jnp.logical_or(r > 0, slot > 0),
                    jnp.logical_or(r < num_rows - 1, slot <= height),
                )
                v = gather.field[owner, slot].astype(F32) * (0.5 * scale) + 0.5 * shift
                v = v + v * jnp.tanh(v)
                hidden_ref[owner, slot] = jnp.where(inside, v, 0.0).astype(BF16)

    def convolve(field, masked, weight_ref, q, beside=None):
        at = at_chip(q)
        one, two = at * 2, at * 2 + 1
        rows = pl.ds(pl.multiple_of(at * 2 * lanes, 2 * lanes), 2 * lanes)
        weights = jnp.concatenate(
            [
                jnp.concatenate([weight_ref[a, b, rows, :] for b in range(3)], axis=1)
                for a in range(3)
            ],
            axis=0,
        )
        tall = 2

        def block(n, _):
            first = n * tall
            keep_up = jnp.logical_or(r > 0, n > 0)
            keep_down = jnp.logical_or(r < num_rows - 1, n < height // tall - 1)
            columns = []
            for a in range(3):
                for p in (one, two):
                    tiles = [field[p, first + a + t] for t in range(tall)]
                    if masked and a == 0:
                        tiles[0] = jnp.where(keep_up, tiles[0], jnp.zeros_like(tiles[0]))
                    if masked and a == 2:
                        tiles[-1] = jnp.where(keep_down, tiles[-1], jnp.zeros_like(tiles[-1]))
                    columns.append(jnp.concatenate(tiles, axis=0))
            product = jnp.dot(
                jnp.concatenate(columns, axis=1), weights, preferred_element_type=F32
            )
            at_rows = pl.ds(pl.multiple_of(first * width, tall * width), tall * width)
            if q == 0:
                total_ref[at_rows, :] = product
            else:
                total_ref[at_rows, :] += product
            if beside is not None:
                beside(n)
            return 0

        lax.fori_loop(0, height // tall, block, 0)

    def shifted_row(i):
        index = lax.broadcasted_iota(jnp.int32, (width, lanes), 0)
        at = slice(i * width, (i + 1) * width)
        before = pltpu.roll(total_ref[at, 0:lanes], 1, axis=0)
        after = pltpu.roll(total_ref[at, 2 * lanes : 3 * lanes], width - 1, axis=0)
        return (
            jnp.where(index == 0, 0.0, before)
            + total_ref[at, lanes : 2 * lanes]
            + jnp.where(index == width - 1, 0.0, after)
        )

    positions = height * width
    count = positions * GROUP_WIDTH

    class Norm:
        def __init__(self, n, gain, bias):
            self.n, self.gain, self.bias = n, gain, bias
            self.centre = self.sums = self.squares = None

        def row(self, i, gather):
            values = shifted_row(i)
            if self.centre is None:
                self.centre = jnp.sum(values, axis=0, keepdims=True) / width
            values = values - self.centre
            gather.field[k, i + gather.off] = values.astype(BF16)
            conv_ref[i * width : (i + 1) * width, :] = values
            total = jnp.sum(values, axis=0, keepdims=True)
            square = jnp.sum(values * values, axis=0, keepdims=True)
            self.sums = total if self.sums is None else self.sums + total
            self.squares = square if self.squares is None else self.squares + square

        def tell(self):
            n = self.n
            mean = group_sum(self.sums + positions * self.centre) / count
            off = self.centre - mean
            square = group_sum(self.squares + 2 * off * self.sums + positions * off * off)
            both = jnp.concatenate([mean, square, self.centre, self.centre], axis=0)
            stat_send[n] = both
            stat_all[n, 0] = both

            def one(d, _):
                pltpu.make_async_remote_copy(
                    src_ref=stat_send.at[n],
                    dst_ref=stat_all.at[n, d],
                    send_sem=stat_send_sems.at[n],
                    recv_sem=stat_recv_sems.at[n],
                    device_id={"rows": lax.rem(r + d, num_rows)},
                    device_id_type=MESH,
                ).start()
                return 0

            lax.fori_loop(1, num_rows, one, 0)

        def coef(self, d):
            n = self.n
            return pltpu.make_async_remote_copy(
                src_ref=coef_send.at[n],
                dst_ref=coef_all.at[n, d],
                send_sem=coef_send_sems.at[n, d],
                recv_sem=coef_recv_sems.at[n, d],
                device_id={"cols": lax.rem(k + d, num_cols)},
                device_id_type=MESH,
            )

        def settle(self):
            n = self.n
            everything = stat_all.at[n, pl.ds(1, num_rows - 1)]
            arrived = pltpu.make_async_remote_copy(
                src_ref=everything,
                dst_ref=everything,
                send_sem=stat_send_sems.at[n],
                recv_sem=stat_recv_sems.at[n],
                device_id={"rows": above},
                device_id_type=MESH,
            )
            arrived.wait_recv()
            pending.append(arrived)
            means = stat_all[n, :, 0, :]
            mean = jnp.sum(means, axis=0, keepdims=True) / num_rows
            spread = means - mean
            square = jnp.sum(stat_all[n, :, 1, :], axis=0, keepdims=True)
            square = square + count * jnp.sum(spread * spread, axis=0, keepdims=True)
            variance = square / (count * num_rows)
            scale = self.gain[...] / jnp.sqrt(variance + 1e-5)
            centres = [stat_all[n, d, 2:3, :] for d in (1, 0, num_rows - 1)]
            shifts = [(c - mean) * scale + self.bias[...] for c in centres]
            rows = jnp.concatenate([scale] + shifts, axis=0)
            coef_send[n] = rows
            coef_all[n, 0] = rows
            for d in range(1, num_cols):
                self.coef(d).start()

        def ready(self):
            for d in range(1, num_cols):
                self.coef(d).wait_recv()
                pending.append(self.coef(d))

    first = Gather(0, field_one, True)

    def look_up(i):
        unroll = 16

        def some(n, _):
            base = n * unroll
            line = i * parts + base // 128
            lane = lax.rem(base, 128)
            for u in range(unroll):
                row = ids_smem[line, lane + u]
                looked_ref[pl.ds(base + u, 1), :] = wide_ref[pl.ds(row, 1), :]
            return 0

        lax.fori_loop(0, width // unroll, some, 0)
        first.field[k, i + 1] = looked_ref[...].astype(BF16)

    for i in range(height):
        look_up(i)
    pl.semaphore_wait(barrier, num_rows - 1 + num_cols - 1)

    def open_gather(gather, make):
        for i in (0, 3, 1, 2):
            make(i)
            if i != 2:
                gather.own_right(i)
            if i != 1:
                gather.own_left(i)
            gather.own(i)

    def pass_on(gather):
        gather.from_left(0)
        gather.from_right(3)
        gather.own_right(2)
        gather.own_left(1)
        if gather.halo:
            gather.halo_in(0)
        gather.from_left(1)
        gather.from_right(2)

    def pass_more(gather):
        gather.from_left(3)
        gather.from_right(0)
        gather.from_far(0)
        gather.from_far(3)
        gather.from_left(2)
        gather.from_right(1)
        if gather.halo:
            gather.halo_in(1)
            gather.halo_in(2)

    def pass_last(gather):
        gather.from_far(1)
        gather.from_far(2)
        if gather.halo:
            gather.halo_in(3)

    open_gather(first, lambda i: None)
    pass_on(first)
    first.rest(0)
    loads[1].wait()
    convolve(field_one, True, conv_one_ref, 0)
    pass_more(first)
    first.rest(1)
    convolve(field_one, True, conv_one_ref, 1)
    pass_last(first)
    first.rest(2)
    convolve(field_one, True, conv_one_ref, 2)
    first.rest(3)
    convolve(field_one, True, conv_one_ref, 3)

    second = Gather(1, field_two, True)
    norm_one = Norm(0, gain_one_ref, bias_one_ref)
    open_gather(second, lambda i: norm_one.row(i, second))
    norm_one.tell()
    pass_on(second)
    norm_one.settle()
    pass_more(second)
    second.rest(0)
    loads[2].wait()
    norm_one.ready()

    def part(q):
        deep = (height + 2) // 2
        return lambda n: normalise(second, q, [n * deep + j for j in range(deep)])

    def normalise_all(q):
        def some(n, _):
            part(q)(n)
            return 0

        lax.fori_loop(0, 2, some, 0)

    normalise_all(0)
    convolve(hidden_ref, False, conv_two_ref, 0)
    pass_last(second)
    second.rest(1)
    normalise_all(1)
    second.rest(2)
    convolve(hidden_ref, False, conv_two_ref, 1, part(2))
    second.rest(3)
    convolve(hidden_ref, False, conv_two_ref, 2, part(3))
    convolve(hidden_ref, False, conv_two_ref, 3)

    third = Gather(2, field_three, False)
    norm_two = Norm(1, gain_two_ref, bias_two_ref)
    open_gather(third, lambda i: norm_two.row(i, third))
    norm_two.tell()
    pass_on(third)
    norm_two.settle()
    scale_two = coef_all[1, 0, 0:1, :]
    shift_two = coef_all[1, 0, 2:3, :]
    for i in range(height):
        v = conv_ref[i * width : (i + 1) * width, :] * scale_two + shift_two
        features_ref[i] = (first.field[k, i + 1].astype(F32) + v).astype(BF16)

    vocab_here = head_hbm.shape[1]
    tiles = vocab_here // 128

    def head_row(i):
        columns = []
        for p in range(num_cols):
            d = lax.rem(k - p + num_cols, num_cols)
            v = third.field[p, i].astype(F32) * coef_all[1, d, 0:1, :] + coef_all[1, d, 2:3, :]
            columns.append((first.field[p, i + 1].astype(F32) + v).astype(BF16))
        left_side = jnp.concatenate(columns, axis=1)
        logits_ref[...] = jnp.dot(left_side, head_ref[...], preferred_element_type=F32)
        most = logits_ref[:, 0:128]
        for t in range(1, tiles):
            most = jnp.maximum(most, logits_ref[:, 128 * t : 128 * t + 128])
        top = jnp.max(most, axis=1, keepdims=True)
        token = tokens_ref[i]
        lane = lax.broadcasted_iota(jnp.int32, (width, 128), 1)
        summed = jnp.zeros((width, 128), F32)
        picked = jnp.zeros((width, 128), F32)
        for t in range(tiles):
            part = logits_ref[:, 128 * t : 128 * t + 128]
            summed = summed + jnp.exp(part - top)
            ids = (lane + (k * vocab_here + 128 * t)).astype(F32)
            picked = picked + jnp.where(ids == token, part, 0.0)
        top_row = jnp.max(most.T, axis=0, keepdims=True)
        sum_row = jnp.sum(summed.T, axis=0, keepdims=True)
        pick_row = jnp.sum(picked.T, axis=0, keepdims=True)
        for s, row in enumerate((top_row, sum_row, pick_row)):
            for b in range(parts):
                last_send[b, s, pl.ds(i, 1), :] = row[:, 128 * b : 128 * b + 128]

    def head_rows(start, step):
        def one(n, _):
            head_row(start + step * n)
            return 0

        lax.fori_loop(0, 2, one, 0)

    def partner_rows(rows):
        for q in range(4):
            for i in rows:
                third.wait((OWN, FROM_P, FROM_M, FAR)[q], i, third.owner_of(q, 1 - core), i)

    pass_more(third)
    partner_rows((0, 3))
    loads[3].wait()
    norm_two.ready()
    head_rows(0, 3)
    pass_last(third)
    partner_rows((1, 2))
    head_rows(1, 1)

    per_block = num_cols // parts

    def exchange(d):
        to = lax.rem(k + d, num_cols)
        return pltpu.make_async_remote_copy(
            src_ref=last_send.at[to // per_block],
            dst_ref=last_all.at[d],
            send_sem=last_send_sems.at[d],
            recv_sem=last_recv_sems.at[d],
            device_id={"cols": to},
            device_id_type=MESH,
        )

    for d in range(1, num_cols):
        exchange(d).start()
    last_all[0] = last_send[k // per_block]
    for d in range(1, num_cols):
        exchange(d).wait_recv()
    top = last_all[0, 0]
    for d in range(1, num_cols):
        top = jnp.maximum(top, last_all[d, 0])
    summed = jnp.zeros_like(top)
    picked = jnp.zeros_like(top)
    for d in range(num_cols):
        summed = summed + last_all[d, 1] * jnp.exp(last_all[d, 0] - top)
        picked = picked + last_all[d, 2]
    logp = picked - top - jnp.log(summed)
    mine = width // num_cols
    place = lax.rem(k, per_block)
    out = logp[:, 0:mine]
    for b in range(1, per_block):
        out = jnp.where(place == b, logp[:, mine * b : mine * b + mine], out)
    logp_ref[...] = out

    for copy in pending:
        copy.wait_send()
    for d in range(1, num_cols):
        exchange(d).wait_send()


def local(
    token_ids,
    keep_mask,
    remask_order,
    embed_table,
    mask_embed,
    conv_one,
    gain_one,
    bias_one,
    conv_two,
    gain_two,
    bias_two,
    head_weight,
):
    num_rows, num_cols = lax.axis_size("rows"), lax.axis_size("cols")
    height, width = token_ids.shape
    vocab, lanes = embed_table.shape
    lines = height * width // 128
    in_vmem = pl.BlockSpec(memory_space=pltpu.VMEM)
    anywhere = pl.BlockSpec(memory_space=pl.ANY)
    return pl.pallas_call(
        functools.partial(kernel, num_rows, num_cols),
        name="denoise",
        out_shape=(
            jax.ShapeDtypeStruct((height, width, lanes), BF16),
            jax.ShapeDtypeStruct((height, width // num_cols), F32),
        ),
        in_specs=[
            in_vmem,
            in_vmem,
            in_vmem,
            anywhere,
            in_vmem,
            anywhere,
            in_vmem,
            in_vmem,
            anywhere,
            in_vmem,
            in_vmem,
            anywhere,
        ],
        out_specs=(in_vmem, in_vmem),
        scratch_shapes=[
            pltpu.VMEM((vocab, lanes), BF16),
            pltpu.VMEM((vocab + 8, lanes), F32),
            pltpu.VMEM(conv_one.shape, BF16),
            pltpu.VMEM(conv_two.shape, BF16),
            pltpu.VMEM(head_weight.shape, BF16),
            pltpu.VMEM((lines, 128), jnp.int32),
            pltpu.SMEM((lines, 128), jnp.int32),
            pltpu.VMEM((height, width, 128), F32),
            pltpu.VMEM((width, lanes), F32),
            pltpu.VMEM((num_cols, height + 2, width, lanes), BF16),
            pltpu.VMEM((num_cols, height + 2, width, lanes), BF16),
            pltpu.VMEM((num_cols, height, width, lanes), BF16),
            pltpu.VMEM((height * width, 3 * lanes), F32),
            pltpu.VMEM((height * width, lanes), F32),
            pltpu.VMEM((2, 4, lanes), F32),
            pltpu.VMEM((2, num_rows, 4, lanes), F32),
            pltpu.VMEM((2, 4, lanes), F32),
            pltpu.VMEM((2, num_cols, 4, lanes), F32),
            pltpu.VMEM((num_cols, height + 2, width, lanes), BF16),
            pltpu.VMEM((width, head_weight.shape[1]), F32),
            pltpu.VMEM((width // 128, 3, height, 128), F32),
            pltpu.VMEM((num_cols, 3, height, 128), F32),
            pltpu.SemaphoreType.DMA((5,)),
            pltpu.SemaphoreType.DMA((3, 11, 4)),
            pltpu.SemaphoreType.DMA((3, 11, 4)),
            pltpu.SemaphoreType.DMA((2,)),
            pltpu.SemaphoreType.DMA((2,)),
            pltpu.SemaphoreType.DMA((2, num_cols)),
            pltpu.SemaphoreType.DMA((2, num_cols)),
            pltpu.SemaphoreType.DMA((num_cols,)),
            pltpu.SemaphoreType.DMA((num_cols,)),
        ],
        compiler_params=pltpu.CompilerParams(
            collective_id=0, has_side_effects=True, vmem_limit_bytes=60 * 1024 * 1024
        ),
    )(
        token_ids,
        keep_mask,
        remask_order.reshape(lines, 128),
        embed_table,
        mask_embed.reshape(1, lanes),
        conv_one,
        gain_one.reshape(1, lanes),
        bias_one.reshape(1, lanes),
        conv_two,
        gain_two.reshape(1, lanes),
        bias_two.reshape(1, lanes),
        head_weight,
    )


def solution(mesh):
    in_specs = (
        P("rows", None),
        P("rows", None),
        P("rows"),
        P(None, "cols"),
        P("cols"),
        P(None, None, None, "cols"),
        P("cols"),
        P("cols"),
        P(None, None, None, "cols"),
        P("cols"),
        P("cols"),
        P(None, "cols"),
    )
    out_specs = (P("rows", None, "cols"), P("rows", "cols"))
    return jax.shard_map(local, mesh=mesh, in_specs=in_specs, out_specs=out_specs, check_vma=False)
```

```python
import functools

import jax
import jax.numpy as jnp
from jax import lax
from jax.experimental import pallas as pl
from jax.experimental.pallas import tpu as pltpu
from jax.sharding import PartitionSpec as P

GROUP_WIDTH = 32
MESH = pl.DeviceIdType.MESH
F32 = jnp.float32
BF16 = jnp.bfloat16
XP, XM, OWN, FROM_P, FROM_M, FAR, FWD, UP, DOWN, UPF, DOWNF = range(11)


def group_sum(row):
    width = row.shape[1]
    a = lax.broadcasted_iota(jnp.int32, (width, width), 0) // GROUP_WIDTH
    b = lax.broadcasted_iota(jnp.int32, (width, width), 1) // GROUP_WIDTH
    ones = jnp.where(a == b, 1.0, 0.0).astype(F32)
    rows = jnp.broadcast_to(row, (8, width))
    return jnp.dot(
        rows, ones, preferred_element_type=F32, precision=lax.Precision.HIGHEST
    )[0:1]


def kernel(
    num_rows,
    num_cols,
    ids_ref,
    keep_ref,
    order_ref,
    table_hbm,
    mask_ref,
    conv_one_hbm,
    gain_one_ref,
    bias_one_ref,
    conv_two_hbm,
    gain_two_ref,
    bias_two_ref,
    head_hbm,
    features_ref,
    logp_ref,
    table_ref,
    wide_ref,
    conv_one_ref,
    conv_two_ref,
    head_ref,
    ids_vmem,
    ids_smem,
    tokens_ref,
    looked_ref,
    field_one,
    field_two,
    field_three,
    total_ref,
    conv_ref,
    stat_send,
    stat_all,
    coef_send,
    coef_all,
    hidden_ref,
    rows_ref,
    logits_ref,
    last_send,
    last_all,
    load_sems,
    send_sems,
    recv_sems,
    stat_send_sems,
    stat_recv_sems,
    coef_send_sems,
    coef_recv_sems,
    last_send_sems,
    last_recv_sems,
    known_sems,
):
    height, width = ids_ref.shape
    vocab = table_hbm.shape[0]
    lanes = table_hbm.shape[1]
    channels = num_cols * lanes
    r = lax.axis_index("rows")
    k = lax.axis_index("cols")
    chips = num_cols // 2
    core = lax.rem(k, 2)
    chip = k // 2
    partner = k + 1 - 2 * core

    def piece(step, c):
        return lax.rem(chip + step, chips) * 2 + c

    right, left = piece(1, core), piece(chips - 1, core)
    above = lax.rem(r + num_rows - 1, num_rows)
    below = lax.rem(r + 1, num_rows)

    loads = [
        pltpu.make_async_copy(src, dst, load_sems.at[n])
        for n, (src, dst) in enumerate(
            (
                (table_hbm, table_ref),
                (conv_one_hbm, conv_one_ref),
                (conv_two_hbm, conv_two_ref),
                (head_hbm, head_ref),
            )
        )
    ]
    loads[0].start()

    barrier = pltpu.get_barrier_semaphore()

    def greet(device):
        pl.semaphore_signal(barrier, inc=1, device_id=device, device_id_type=MESH)

    for d in range(1, num_cols):
        greet({"cols": lax.rem(k + d, num_cols)})
    greet({"rows": above})
    greet({"rows": below})

    def tell_known(m):
        far = 2**m
        for to in (lax.rem(r + far, num_rows), lax.rem(r + num_rows - far, num_rows)):
            pl.semaphore_signal(
                known_sems.at[m], inc=1, device_id={"rows": to}, device_id_type=MESH
            )

    rounds = max(num_rows.bit_length() - 2, 0)

    def meet(m):
        if m < rounds:
            pl.semaphore_wait(known_sems.at[m], 2)
            if m + 1 < rounds:
                tell_known(m + 1)

    half = height * width * num_rows // 2
    parts = width // 128
    for i in range(height):
        for j in range(parts):
            at = (slice(i, i + 1), slice(128 * j, 128 * j + 128))
            n = i * parts + j
            visible = (keep_ref[at] == 1) | (order_ref[n : n + 1, :] >= half)
            ids_vmem[n : n + 1, :] = jnp.where(visible, ids_ref[at], vocab)
    to_smem = pltpu.make_async_copy(ids_vmem, ids_smem, load_sems.at[4])
    to_smem.start()

    def lay_tokens():
        for i in range(height):
            row = ids_ref[i : i + 1, :].astype(F32)
            tokens_ref[i] = jnp.broadcast_to(row, (128, width)).T

    loads[0].wait()
    for load in loads[1:]:
        load.start()
    step_rows = 512

    def widen(n, _):
        at = pl.ds(pl.multiple_of(n * step_rows, step_rows), step_rows)
        wide_ref[at, :] = table_ref[at, :].astype(F32)
        return 0

    lax.fori_loop(0, vocab // step_rows, widen, 0)
    wide_ref[vocab : vocab + 8, :] = jnp.broadcast_to(mask_ref[...].astype(F32), (8, lanes))
    to_smem.wait()

    pending = []

    class Gather:
        def __init__(self, n, field, halo):
            self.n, self.field, self.halo = n, field, halo
            self.off = 1 if halo else 0

        def copy(self, kind, slot, owner, row, device, to_row=None):
            to_row = row if to_row is None else to_row
            return pltpu.make_async_remote_copy(
                src_ref=self.field.at[owner, row],
                dst_ref=self.field.at[owner, to_row],
                send_sem=send_sems.at[self.n, kind, slot],
                recv_sem=recv_sems.at[self.n, kind, slot],
                device_id=device,
                device_id_type=MESH,
            )

        def send(self, *args, **kw):
            c = self.copy(*args, **kw)
            c.start()
            pending.append(c)

        def wait(self, kind, slot, owner, row):
            self.copy(kind, slot, owner, row, {"cols": partner}).wait_recv()

        def halo_out(self, q, owner, i):
            if not self.halo:
                return
            if i == 0:
                self.send(UP, q, owner, 1, {"rows": above}, to_row=height + 1)
            if i == height - 1:
                self.send(DOWN, q, owner, height, {"rows": below}, to_row=0)

        def own(self, i):
            row = i + self.off
            self.halo_out(0, k, i)
            self.send(OWN, i, k, row, {"cols": partner})

        def own_right(self, i):
            self.send(XP, i, k, i + self.off, {"cols": right})

        def own_left(self, i):
            self.send(XM, i, k, i + self.off, {"cols": left})

        def from_left(self, i):
            row, owner = i + self.off, left
            self.wait(XP, i, owner, row)
            if i in (0, 1):
                self.send(FWD, i, owner, row, {"cols": right})
            self.halo_out(1, owner, i)
            self.send(FROM_P, i, owner, row, {"cols": partner})

        def from_right(self, i):
            row, owner = i + self.off, right
            self.wait(XM, i, owner, row)
            if i in (2, 3):
                self.send(FWD, i, owner, row, {"cols": left})
            self.halo_out(2, owner, i)
            self.send(FROM_M, i, owner, row, {"cols": partner})

        def from_far(self, i):
            row, owner = i + self.off, piece(2, core)
            self.wait(FWD, i, owner, row)
            self.halo_out(3, owner, i)
            self.send(FAR, i, owner, row, {"cols": partner})

        def owner_of(self, q, c):
            return piece((0, chips - 1, 1, 2)[q], c)

        def halo_in(self, q):
            owner = self.owner_of(q, core)
            self.wait(UP, q, owner, height + 1)
            self.send(UPF, q, owner, height + 1, {"cols": partner})
            self.wait(DOWN, q, owner, 0)
            self.send(DOWNF, q, owner, 0, {"cols": partner})

        def rest_rows(self, q, rows):
            owner = self.owner_of(q, 1 - core)
            for i in rows:
                self.wait((OWN, FROM_P, FROM_M, FAR)[q], i, owner, i + self.off)

        def rest_halo(self, q):
            owner = self.owner_of(q, 1 - core)
            self.wait(UPF, q, owner, height + 1)
            self.wait(DOWNF, q, owner, 0)

        def rest(self, q):
            self.rest_rows(q, range(height))
            self.rest_halo(q)

    def at_chip(q):
        return lax.rem(chip + (0, chips - 1, 1, 2)[q], chips)

    def normalise(gather, q, slots):
        for c in range(2):
            owner = at_chip(q) * 2 + c
            d = lax.rem(k - owner + num_cols, num_cols)
            scale = coef_all[0, d, 0:1, :]
            for slot in slots:
                which = 1 + jnp.where(slot > 0, 1, 0) + jnp.where(slot > height, 1, 0)
                shift = coef_all[0, d, pl.ds(which, 1), :]
                inside = jnp.logical_and(
                    jnp.logical_or(r > 0, slot > 0),
                    jnp.logical_or(r < num_rows - 1, slot <= height),
                )
                v = gather.field[owner, slot].astype(F32) * (0.5 * scale) + 0.5 * shift
                v = v + v * jnp.tanh(v)
                hidden_ref[owner, slot] = jnp.where(inside, v, 0.0).astype(BF16)

    def convolve(field, masked, weight_ref, q, outs, started=True):
        at = at_chip(q)
        rows = pl.ds(pl.multiple_of(at * 2 * lanes, 2 * lanes), 2 * lanes)
        weights = jnp.concatenate(
            [
                jnp.concatenate([weight_ref[a, b, rows, :] for b in range(3)], axis=1)
                for a in range(3)
            ],
            axis=0,
        )
        columns = []
        for a in range(3):
            for p in (at * 2, at * 2 + 1):
                tiles = []
                for i in outs:
                    tile = field[p, i + a]
                    if masked and i + a == 0:
                        tile = jnp.where(r > 0, tile, jnp.zeros_like(tile))
                    if masked and i + a == height + 1:
                        tile = jnp.where(r < num_rows - 1, tile, jnp.zeros_like(tile))
                    tiles.append(tile)
                columns.append(jnp.concatenate(tiles, axis=0))
        product = jnp.dot(
            jnp.concatenate(columns, axis=1), weights, preferred_element_type=F32
        )
        for n, i in enumerate(outs):
            here = slice(i * width, (i + 1) * width)
            part = product[n * width : (n + 1) * width]
            if started:
                total_ref[here, :] += part
            else:
                total_ref[here, :] = part

    def shifted_row(i):
        index = lax.broadcasted_iota(jnp.int32, (width, lanes), 0)
        at = slice(i * width, (i + 1) * width)
        before = pltpu.roll(total_ref[at, 0:lanes], 1, axis=0)
        after = pltpu.roll(total_ref[at, 2 * lanes : 3 * lanes], width - 1, axis=0)
        return (
            jnp.where(index == 0, 0.0, before)
            + total_ref[at, lanes : 2 * lanes]
            + jnp.where(index == width - 1, 0.0, after)
        )

    positions = height * width
    count = positions * GROUP_WIDTH

    class Norm:
        def __init__(self, n, gain, bias):
            self.n, self.gain, self.bias = n, gain, bias
            self.centre = self.sums = self.squares = None

        def row(self, i, gather):
            values = shifted_row(i)
            if self.centre is None:
                self.centre = jnp.sum(values, axis=0, keepdims=True) / width
            values = values - self.centre
            gather.field[k, i + gather.off] = values.astype(BF16)
            conv_ref[i * width : (i + 1) * width, :] = values
            total = jnp.sum(values, axis=0, keepdims=True)
            square = jnp.sum(values * values, axis=0, keepdims=True)
            self.sums = total if self.sums is None else self.sums + total
            self.squares = square if self.squares is None else self.squares + square

        def tell(self):
            n = self.n
            mean = group_sum(self.sums + positions * self.centre) / count
            off = self.centre - mean
            square = group_sum(self.squares + 2 * off * self.sums + positions * off * off)
            both = jnp.concatenate([mean, square, self.centre, self.centre], axis=0)
            stat_send[n] = both
            stat_all[n, 0] = both

            def one(d, _):
                pltpu.make_async_remote_copy(
                    src_ref=stat_send.at[n],
                    dst_ref=stat_all.at[n, d],
                    send_sem=stat_send_sems.at[n],
                    recv_sem=stat_recv_sems.at[n],
                    device_id={"rows": lax.rem(r + d, num_rows)},
                    device_id_type=MESH,
                ).start()
                return 0

            lax.fori_loop(1, num_rows, one, 0)

        def coef(self, d):
            n = self.n
            return pltpu.make_async_remote_copy(
                src_ref=coef_send.at[n],
                dst_ref=coef_all.at[n, d],
                send_sem=coef_send_sems.at[n, d],
                recv_sem=coef_recv_sems.at[n, d],
                device_id={"cols": lax.rem(k + d, num_cols)},
                device_id_type=MESH,
            )

        def settle(self):
            n = self.n
            everything = stat_all.at[n, pl.ds(1, num_rows - 1)]
            arrived = pltpu.make_async_remote_copy(
                src_ref=everything,
                dst_ref=everything,
                send_sem=stat_send_sems.at[n],
                recv_sem=stat_recv_sems.at[n],
                device_id={"rows": above},
                device_id_type=MESH,
            )
            arrived.wait_recv()
            pending.append(arrived)
            means = stat_all[n, :, 0, :]
            mean = jnp.sum(means, axis=0, keepdims=True) / num_rows
            spread = means - mean
            square = jnp.sum(stat_all[n, :, 1, :], axis=0, keepdims=True)
            square = square + count * jnp.sum(spread * spread, axis=0, keepdims=True)
            variance = square / (count * num_rows)
            scale = self.gain[...] / jnp.sqrt(variance + 1e-5)
            centres = [stat_all[n, d, 2:3, :] for d in (1, 0, num_rows - 1)]
            shifts = [(c - mean) * scale + self.bias[...] for c in centres]
            rows = jnp.concatenate([scale] + shifts, axis=0)
            coef_send[n] = rows
            coef_all[n, 0] = rows
            for d in range(1, num_cols):
                self.coef(d).start()

        def ready(self):
            for d in range(1, num_cols):
                self.coef(d).wait_recv()
                pending.append(self.coef(d))

    first = Gather(0, field_one, True)

    def look_up(i):
        unroll = 16

        def some(n, _):
            base = n * unroll
            line = i * parts + base // 128
            lane = lax.rem(base, 128)
            for u in range(unroll):
                row = ids_smem[line, lane + u]
                looked_ref[pl.ds(base + u, 1), :] = wide_ref[pl.ds(row, 1), :]
            return 0

        lax.fori_loop(0, width // unroll, some, 0)
        first.field[k, i + 1] = looked_ref[...].astype(BF16)

    look_up(0)
    pl.semaphore_wait(barrier, num_cols - 1 + 2)
    if rounds > 0:
        tell_known(0)

    def open_gather(gather, make):
        for i in (0, 3, 1, 2):
            make(i)
            if i != 2:
                gather.own_right(i)
            if i != 1:
                gather.own_left(i)
            gather.own(i)

    def pass_on(gather):
        gather.from_left(0)
        gather.from_right(3)
        gather.own_right(2)
        gather.own_left(1)
        if gather.halo:
            gather.halo_in(0)
        gather.from_left(1)
        gather.from_right(2)

    inner, outer, every = (1, 2), (0, 3), (0, 1, 2, 3)

    open_gather(first, lambda i: look_up(i) if i > 0 else None)
    pass_on(first)
    meet(0)
    lay_tokens()
    first.rest(0)
    loads[1].wait()
    convolve(field_one, True, conv_one_ref, 0, every, False)
    meet(1)
    first.from_left(3)
    first.from_right(0)
    first.from_far(0)
    first.from_far(3)
    meet(2)
    first.from_left(2)
    first.from_right(1)
    first.halo_in(1)
    first.halo_in(2)
    meet(3)
    first.rest_rows(1, every)
    convolve(field_one, True, conv_one_ref, 1, inner)
    first.from_far(1)
    first.from_far(2)
    first.rest_rows(2, every)
    convolve(field_one, True, conv_one_ref, 2, inner)
    first.halo_in(3)
    first.rest_halo(1)
    convolve(field_one, True, conv_one_ref, 1, outer)
    first.rest_halo(2)
    convolve(field_one, True, conv_one_ref, 2, outer)
    first.rest(3)
    convolve(field_one, True, conv_one_ref, 3, every)

    second = Gather(1, field_two, True)
    norm_one = Norm(0, gain_one_ref, bias_one_ref)
    open_gather(second, lambda i: norm_one.row(i, second))
    norm_one.tell()
    pass_on(second)
    norm_one.settle()
    second.from_left(3)
    second.from_right(0)
    second.from_far(0)
    second.from_far(3)
    second.from_left(2)
    second.from_right(1)
    second.halo_in(1)
    second.halo_in(2)
    second.rest(0)
    loads[2].wait()
    norm_one.ready()
    slots = range(height + 2)
    normalise(second, 0, slots)
    second.from_far(1)
    second.from_far(2)
    second.rest(1)
    normalise(second, 1, slots)
    convolve(hidden_ref, False, conv_two_ref, 0, every, False)
    second.halo_in(3)
    second.rest(2)
    normalise(second, 2, slots)
    convolve(hidden_ref, False, conv_two_ref, 1, every)
    second.rest(3)
    normalise(second, 3, slots)
    convolve(hidden_ref, False, conv_two_ref, 2, every)
    convolve(hidden_ref, False, conv_two_ref, 3, every)

    third = Gather(2, field_three, False)
    norm_two = Norm(1, gain_two_ref, bias_two_ref)
    open_gather(third, lambda i: norm_two.row(i, third))
    norm_two.tell()
    pass_on(third)
    norm_two.settle()
    scale_two = coef_all[1, 0, 0:1, :]
    shift_two = coef_all[1, 0, 2:3, :]
    for i in range(height):
        v = conv_ref[i * width : (i + 1) * width, :] * scale_two + shift_two
        features_ref[i] = (first.field[k, i + 1].astype(F32) + v).astype(BF16)

    vocab_here = head_hbm.shape[1]
    tiles = vocab_here // 128

    def all_features(i, to):
        for p in range(num_cols):
            d = lax.rem(k - p + num_cols, num_cols)
            v = third.field[p, i].astype(F32) * coef_all[1, d, 0:1, :] + coef_all[1, d, 2:3, :]
            v = first.field[p, i + 1].astype(F32) + v
            rows_ref[to, :, p * lanes : (p + 1) * lanes] = v.astype(BF16)

    def row_logits(to):
        logits_ref[to] = jnp.dot(rows_ref[to], head_ref[...], preferred_element_type=F32)

    def row_totals(i, to):
        most = logits_ref[to, :, 0:128]
        for t in range(1, tiles):
            most = jnp.maximum(most, logits_ref[to, :, 128 * t : 128 * t + 128])
        top = jnp.max(most, axis=1, keepdims=True)
        token = tokens_ref[i]
        lane = lax.broadcasted_iota(jnp.int32, (width, 128), 1)
        summed = jnp.zeros((width, 128), F32)
        picked = jnp.zeros((width, 128), F32)
        for t in range(tiles):
            part = logits_ref[to, :, 128 * t : 128 * t + 128]
            summed = summed + jnp.exp(part - top)
            ids = (lane + (k * vocab_here + 128 * t)).astype(F32)
            picked = picked + jnp.where(ids == token, part, 0.0)
        top_row = jnp.max(most.T, axis=0, keepdims=True)
        sum_row = jnp.sum(summed.T, axis=0, keepdims=True)
        pick_row = jnp.sum(picked.T, axis=0, keepdims=True)
        for n, row in enumerate((top_row, sum_row, pick_row)):
            for b in range(parts):
                last_send[b, n, i : i + 1, :] = row[:, 128 * b : 128 * b + 128]

    third.from_left(3)
    third.from_right(0)
    third.from_far(0)
    third.from_far(3)
    third.from_left(2)
    third.from_right(1)
    for q in range(4):
        third.rest_rows(q, (0, 3))
    loads[3].wait()
    norm_two.ready()
    all_features(0, 0)
    row_logits(0)
    all_features(3, 1)
    third.from_far(1)
    third.from_far(2)
    row_logits(1)
    row_totals(0, 0)
    for q in range(4):
        third.rest_rows(q, (1, 2))
    all_features(1, 0)
    row_logits(0)
    row_totals(3, 1)
    all_features(2, 1)
    row_logits(1)
    row_totals(1, 0)
    row_totals(2, 1)

    per_block = num_cols // parts

    def exchange(d):
        to = lax.rem(k + d, num_cols)
        return pltpu.make_async_remote_copy(
            src_ref=last_send.at[to // per_block],
            dst_ref=last_all.at[d],
            send_sem=last_send_sems.at[d],
            recv_sem=last_recv_sems.at[d],
            device_id={"cols": to},
            device_id_type=MESH,
        )

    for d in range(1, num_cols):
        exchange(d).start()
    last_all[0] = last_send[k // per_block]
    for d in range(1, num_cols):
        exchange(d).wait_recv()
    top = last_all[0, 0]
    for d in range(1, num_cols):
        top = jnp.maximum(top, last_all[d, 0])
    summed = jnp.zeros_like(top)
    picked = jnp.zeros_like(top)
    for d in range(num_cols):
        summed = summed + last_all[d, 1] * jnp.exp(last_all[d, 0] - top)
        picked = picked + last_all[d, 2]
    logp = picked - top - jnp.log(summed)
    mine = width // num_cols
    place = lax.rem(k, per_block)
    out = logp[:, 0:mine]
    for b in range(1, per_block):
        out = jnp.where(place == b, logp[:, mine * b : mine * b + mine], out)
    logp_ref[...] = out

    for copy in pending:
        copy.wait_send()
    for d in range(1, num_cols):
        exchange(d).wait_send()


def local(
    token_ids,
    keep_mask,
    remask_order,
    embed_table,
    mask_embed,
    conv_one,
    gain_one,
    bias_one,
    conv_two,
    gain_two,
    bias_two,
    head_weight,
):
    num_rows, num_cols = lax.axis_size("rows"), lax.axis_size("cols")
    height, width = token_ids.shape
    vocab, lanes = embed_table.shape
    lines = height * width // 128
    in_vmem = pl.BlockSpec(memory_space=pltpu.VMEM)
    anywhere = pl.BlockSpec(memory_space=pl.ANY)
    return pl.pallas_call(
        functools.partial(kernel, num_rows, num_cols),
        name="denoise",
        out_shape=(
            jax.ShapeDtypeStruct((height, width, lanes), BF16),
            jax.ShapeDtypeStruct((height, width // num_cols), F32),
        ),
        in_specs=[
            in_vmem,
            in_vmem,
            in_vmem,
            anywhere,
            in_vmem,
            anywhere,
            in_vmem,
            in_vmem,
            anywhere,
            in_vmem,
            in_vmem,
            anywhere,
        ],
        out_specs=(in_vmem, in_vmem),
        scratch_shapes=[
            pltpu.VMEM((vocab, lanes), BF16),
            pltpu.VMEM((vocab + 8, lanes), F32),
            pltpu.VMEM(conv_one.shape, BF16),
            pltpu.VMEM(conv_two.shape, BF16),
            pltpu.VMEM(head_weight.shape, BF16),
            pltpu.VMEM((lines, 128), jnp.int32),
            pltpu.SMEM((lines, 128), jnp.int32),
            pltpu.VMEM((height, width, 128), F32),
            pltpu.VMEM((width, lanes), F32),
            pltpu.VMEM((num_cols, height + 2, width, lanes), BF16),
            pltpu.VMEM((num_cols, height + 2, width, lanes), BF16),
            pltpu.VMEM((num_cols, height, width, lanes), BF16),
            pltpu.VMEM((height * width, 3 * lanes), F32),
            pltpu.VMEM((height * width, lanes), F32),
            pltpu.VMEM((2, 4, lanes), F32),
            pltpu.VMEM((2, num_rows, 4, lanes), F32),
            pltpu.VMEM((2, 4, lanes), F32),
            pltpu.VMEM((2, num_cols, 4, lanes), F32),
            pltpu.VMEM((num_cols, height + 2, width, lanes), BF16),
            pltpu.VMEM((2, width, num_cols * lanes), BF16),
            pltpu.VMEM((2, width, head_weight.shape[1]), F32),
            pltpu.VMEM((width // 128, 3, height, 128), F32),
            pltpu.VMEM((num_cols, 3, height, 128), F32),
            pltpu.SemaphoreType.DMA((5,)),
            pltpu.SemaphoreType.DMA((3, 11, 4)),
            pltpu.SemaphoreType.DMA((3, 11, 4)),
            pltpu.SemaphoreType.DMA((2,)),
            pltpu.SemaphoreType.DMA((2,)),
            pltpu.SemaphoreType.DMA((2, num_cols)),
            pltpu.SemaphoreType.DMA((2, num_cols)),
            pltpu.SemaphoreType.DMA((num_cols,)),
            pltpu.SemaphoreType.DMA((num_cols,)),
            pltpu.SemaphoreType.REGULAR((8,)),
        ],
        compiler_params=pltpu.CompilerParams(
            collective_id=0, has_side_effects=True, vmem_limit_bytes=60 * 1024 * 1024
        ),
    )(
        token_ids,
        keep_mask,
        remask_order.reshape(lines, 128),
        embed_table,
        mask_embed.reshape(1, lanes),
        conv_one,
        gain_one.reshape(1, lanes),
        bias_one.reshape(1, lanes),
        conv_two,
        gain_two.reshape(1, lanes),
        bias_two.reshape(1, lanes),
        head_weight,
    )


def solution(mesh):
    in_specs = (
        P("rows", None),
        P("rows", None),
        P("rows"),
        P(None, "cols"),
        P("cols"),
        P(None, None, None, "cols"),
        P("cols"),
        P("cols"),
        P(None, None, None, "cols"),
        P("cols"),
        P("cols"),
        P(None, "cols"),
    )
    out_specs = (P("rows", None, "cols"), P("rows", "cols"))
    return jax.shard_map(local, mesh=mesh, in_specs=in_specs, out_specs=out_specs, check_vma=False)
```

```python
import functools

import jax
import jax.numpy as jnp
from jax import lax
from jax.experimental import pallas as pl
from jax.experimental.pallas import tpu as pltpu
from jax.sharding import PartitionSpec as P

GROUP_WIDTH = 32
MESH = pl.DeviceIdType.MESH
F32 = jnp.float32
BF16 = jnp.bfloat16
XP, XM, OWN, FROM_P, FROM_M, FAR, FWD, UP, DOWN, UPF, DOWNF = range(11)


def group_sum(row):
    width = row.shape[1]
    a = lax.broadcasted_iota(jnp.int32, (width, width), 0) // GROUP_WIDTH
    b = lax.broadcasted_iota(jnp.int32, (width, width), 1) // GROUP_WIDTH
    ones = jnp.where(a == b, 1.0, 0.0).astype(F32)
    rows = jnp.broadcast_to(row, (8, width))
    return jnp.dot(
        rows, ones, preferred_element_type=F32, precision=lax.Precision.HIGHEST
    )[0:1]


def kernel(
    num_rows,
    num_cols,
    ids_ref,
    keep_ref,
    order_ref,
    table_hbm,
    mask_ref,
    conv_one_hbm,
    gain_one_ref,
    bias_one_ref,
    conv_two_hbm,
    gain_two_ref,
    bias_two_ref,
    head_hbm,
    features_ref,
    totals_ref,
    table_ref,
    wide_ref,
    conv_one_ref,
    conv_two_ref,
    head_ref,
    ids_vmem,
    ids_smem,
    tokens_ref,
    looked_ref,
    field_one,
    field_two,
    field_three,
    total_ref,
    conv_ref,
    stat_send,
    stat_all,
    coef_send,
    coef_all,
    hidden_ref,
    rows_ref,
    logits_ref,
    last_send,
    last_all,
    load_sems,
    send_sems,
    recv_sems,
    stat_send_sems,
    stat_recv_sems,
    coef_send_sems,
    coef_recv_sems,
    last_send_sems,
    last_recv_sems,
    known_sems,
):
    height, width = ids_ref.shape
    vocab = table_hbm.shape[0]
    lanes = table_hbm.shape[1]
    channels = num_cols * lanes
    r = lax.axis_index("rows")
    k = lax.axis_index("cols")
    chips = num_cols // 2
    core = lax.rem(k, 2)
    chip = k // 2
    partner = k + 1 - 2 * core

    def piece(step, c):
        return lax.rem(chip + step, chips) * 2 + c

    right, left = piece(1, core), piece(chips - 1, core)
    above = lax.rem(r + num_rows - 1, num_rows)
    below = lax.rem(r + 1, num_rows)

    loads = [
        pltpu.make_async_copy(src, dst, load_sems.at[n])
        for n, (src, dst) in enumerate(
            (
                (table_hbm, table_ref),
                (conv_one_hbm, conv_one_ref),
                (conv_two_hbm, conv_two_ref),
                (head_hbm, head_ref),
            )
        )
    ]
    loads[0].start()

    barrier = pltpu.get_barrier_semaphore()

    def greet(device):
        pl.semaphore_signal(barrier, inc=1, device_id=device, device_id_type=MESH)

    for d in range(1, num_cols):
        greet({"cols": lax.rem(k + d, num_cols)})
    greet({"rows": above})
    greet({"rows": below})

    def tell_known(m):
        far = 2**m
        for to in (lax.rem(r + far, num_rows), lax.rem(r + num_rows - far, num_rows)):
            pl.semaphore_signal(
                known_sems.at[m], inc=1, device_id={"rows": to}, device_id_type=MESH
            )

    rounds = max(num_rows.bit_length() - 2, 0)

    def meet(m):
        if m < rounds:
            pl.semaphore_wait(known_sems.at[m], 2)
            if m + 1 < rounds:
                tell_known(m + 1)

    half = height * width * num_rows // 2
    parts = width // 128
    for i in range(height):
        for j in range(parts):
            at = (slice(i, i + 1), slice(128 * j, 128 * j + 128))
            n = i * parts + j
            visible = (keep_ref[at] == 1) | (order_ref[n : n + 1, :] >= half)
            ids_vmem[n : n + 1, :] = jnp.where(visible, ids_ref[at], vocab)
    to_smem = pltpu.make_async_copy(ids_vmem, ids_smem, load_sems.at[4])
    to_smem.start()

    def lay_tokens():
        for i in range(height):
            row = ids_ref[i : i + 1, :].astype(F32)
            tokens_ref[i] = jnp.broadcast_to(row, (128, width)).T

    loads[0].wait()
    for load in loads[1:]:
        load.start()
    step_rows = 512

    def widen(n, _):
        at = pl.ds(pl.multiple_of(n * step_rows, step_rows), step_rows)
        wide_ref[at, :] = table_ref[at, :].astype(F32)
        return 0

    lax.fori_loop(0, vocab // step_rows, widen, 0)
    wide_ref[vocab : vocab + 8, :] = jnp.broadcast_to(mask_ref[...].astype(F32), (8, lanes))
    to_smem.wait()

    pending = []

    class Gather:
        def __init__(self, n, field, halo):
            self.n, self.field, self.halo = n, field, halo
            self.off = 1 if halo else 0

        def copy(self, kind, slot, owner, row, device, to_row=None):
            to_row = row if to_row is None else to_row
            return pltpu.make_async_remote_copy(
                src_ref=self.field.at[owner, row],
                dst_ref=self.field.at[owner, to_row],
                send_sem=send_sems.at[self.n, kind, slot],
                recv_sem=recv_sems.at[self.n, kind, slot],
                device_id=device,
                device_id_type=MESH,
            )

        def send(self, *args, **kw):
            c = self.copy(*args, **kw)
            c.start()
            pending.append(c)

        def wait(self, kind, slot, owner, row):
            self.copy(kind, slot, owner, row, {"cols": partner}).wait_recv()

        def halo_out(self, q, owner, i):
            if not self.halo:
                return
            if i == 0:
                self.send(UP, q, owner, 1, {"rows": above}, to_row=height + 1)
            if i == height - 1:
                self.send(DOWN, q, owner, height, {"rows": below}, to_row=0)

        def own(self, i):
            self.send(OWN, i, k, i + self.off, {"cols": partner})

        def own_right(self, i):
            self.send(XP, i, k, i + self.off, {"cols": right})

        def own_left(self, i):
            self.send(XM, i, k, i + self.off, {"cols": left})

        def from_left(self, i):
            row, owner = i + self.off, left
            self.wait(XP, i, owner, row)
            if i in (0, 1):
                self.send(FWD, i, owner, row, {"cols": right})
            self.halo_out(1, owner, i)
            self.send(FROM_P, i, owner, row, {"cols": partner})

        def from_right(self, i):
            row, owner = i + self.off, right
            self.wait(XM, i, owner, row)
            if i in (2, 3):
                self.send(FWD, i, owner, row, {"cols": left})
            self.halo_out(2, owner, i)
            self.send(FROM_M, i, owner, row, {"cols": partner})

        def from_far(self, i):
            row, owner = i + self.off, piece(2, core)
            self.wait(FWD, i, owner, row)
            self.halo_out(3, owner, i)
            self.send(FAR, i, owner, row, {"cols": partner})

        def owner_of(self, q, c):
            return piece((0, chips - 1, 1, 2)[q], c)

        def halo_in(self, q):
            owner = self.owner_of(q, core)
            self.wait(UP, q, owner, height + 1)
            self.send(UPF, q, owner, height + 1, {"cols": partner})
            self.wait(DOWN, q, owner, 0)
            self.send(DOWNF, q, owner, 0, {"cols": partner})

        def rest_rows(self, q, rows):
            owner = self.owner_of(q, 1 - core)
            for i in rows:
                self.wait((OWN, FROM_P, FROM_M, FAR)[q], i, owner, i + self.off)

        def rest_halo(self, q):
            owner = self.owner_of(q, 1 - core)
            self.wait(UPF, q, owner, height + 1)
            self.wait(DOWNF, q, owner, 0)

        def rest(self, q):
            self.rest_rows(q, range(height))
            self.rest_halo(q)

    def at_chip(q):
        return lax.rem(chip + (0, chips - 1, 1, 2)[q], chips)

    def normalise(gather, q, slots):
        for c in range(2):
            owner = at_chip(q) * 2 + c
            d = lax.rem(k - owner + num_cols, num_cols)
            scale = coef_all[0, d, 0:1, :]
            for slot in slots:
                which = 1 + jnp.where(slot > 0, 1, 0) + jnp.where(slot > height, 1, 0)
                shift = coef_all[0, d, pl.ds(which, 1), :]
                inside = jnp.logical_and(
                    jnp.logical_or(r > 0, slot > 0),
                    jnp.logical_or(r < num_rows - 1, slot <= height),
                )
                v = gather.field[owner, slot].astype(F32) * (0.5 * scale) + 0.5 * shift
                v = v + v * jnp.tanh(v)
                hidden_ref[owner, slot] = jnp.where(inside, v, 0.0).astype(BF16)

    def convolve(field, masked, weight_ref, q, outs, started=True):
        at = at_chip(q)
        rows = pl.ds(pl.multiple_of(at * 2 * lanes, 2 * lanes), 2 * lanes)
        weights = jnp.concatenate(
            [
                jnp.concatenate([weight_ref[a, b, rows, :] for b in range(3)], axis=1)
                for a in range(3)
            ],
            axis=0,
        )
        columns = []
        for a in range(3):
            for p in (at * 2, at * 2 + 1):
                tiles = []
                for i in outs:
                    tile = field[p, i + a]
                    if masked and i + a == 0:
                        tile = jnp.where(r > 0, tile, jnp.zeros_like(tile))
                    if masked and i + a == height + 1:
                        tile = jnp.where(r < num_rows - 1, tile, jnp.zeros_like(tile))
                    tiles.append(tile)
                columns.append(jnp.concatenate(tiles, axis=0))
        product = jnp.dot(
            jnp.concatenate(columns, axis=1), weights, preferred_element_type=F32
        )
        for n, i in enumerate(outs):
            here = slice(i * width, (i + 1) * width)
            part = product[n * width : (n + 1) * width]
            if started:
                total_ref[here, :] += part
            else:
                total_ref[here, :] = part

    def shifted_row(i):
        index = lax.broadcasted_iota(jnp.int32, (width, lanes), 0)
        at = slice(i * width, (i + 1) * width)
        before = pltpu.roll(total_ref[at, 0:lanes], 1, axis=0)
        after = pltpu.roll(total_ref[at, 2 * lanes : 3 * lanes], width - 1, axis=0)
        return (
            jnp.where(index == 0, 0.0, before)
            + total_ref[at, lanes : 2 * lanes]
            + jnp.where(index == width - 1, 0.0, after)
        )

    positions = height * width
    count = positions * GROUP_WIDTH

    class Norm:
        def __init__(self, n, gain, bias):
            self.n, self.gain, self.bias = n, gain, bias
            self.centre = self.sums = self.squares = None

        def row(self, i, gather):
            values = shifted_row(i)
            if self.centre is None:
                self.centre = jnp.sum(values, axis=0, keepdims=True) / width
            values = values - self.centre
            gather.field[k, i + gather.off] = values.astype(BF16)
            conv_ref[i * width : (i + 1) * width, :] = values
            total = jnp.sum(values, axis=0, keepdims=True)
            square = jnp.sum(values * values, axis=0, keepdims=True)
            self.sums = total if self.sums is None else self.sums + total
            self.squares = square if self.squares is None else self.squares + square

        def tell(self):
            n = self.n
            mean = group_sum(self.sums + positions * self.centre) / count
            off = self.centre - mean
            square = group_sum(self.squares + 2 * off * self.sums + positions * off * off)
            both = jnp.concatenate([mean, square, self.centre, self.centre], axis=0)
            stat_send[n] = both
            stat_all[n, 0] = both

            def one(d, _):
                pltpu.make_async_remote_copy(
                    src_ref=stat_send.at[n],
                    dst_ref=stat_all.at[n, d],
                    send_sem=stat_send_sems.at[n],
                    recv_sem=stat_recv_sems.at[n],
                    device_id={"rows": lax.rem(r + d, num_rows)},
                    device_id_type=MESH,
                ).start()
                return 0

            lax.fori_loop(1, num_rows, one, 0)

        def coef(self, d):
            n = self.n
            return pltpu.make_async_remote_copy(
                src_ref=coef_send.at[n],
                dst_ref=coef_all.at[n, d],
                send_sem=coef_send_sems.at[n, d],
                recv_sem=coef_recv_sems.at[n, d],
                device_id={"cols": lax.rem(k + d, num_cols)},
                device_id_type=MESH,
            )

        def settle(self):
            n = self.n
            everything = stat_all.at[n, pl.ds(1, num_rows - 1)]
            arrived = pltpu.make_async_remote_copy(
                src_ref=everything,
                dst_ref=everything,
                send_sem=stat_send_sems.at[n],
                recv_sem=stat_recv_sems.at[n],
                device_id={"rows": above},
                device_id_type=MESH,
            )
            arrived.wait_recv()
            pending.append(arrived)
            means = stat_all[n, :, 0, :]
            mean = jnp.sum(means, axis=0, keepdims=True) / num_rows
            spread = means - mean
            square = jnp.sum(stat_all[n, :, 1, :], axis=0, keepdims=True)
            square = square + count * jnp.sum(spread * spread, axis=0, keepdims=True)
            variance = square / (count * num_rows)
            scale = self.gain[...] / jnp.sqrt(variance + 1e-5)
            centres = [stat_all[n, d, 2:3, :] for d in (1, 0, num_rows - 1)]
            shifts = [(c - mean) * scale + self.bias[...] for c in centres]
            rows = jnp.concatenate([scale] + shifts, axis=0)
            coef_send[n] = rows
            coef_all[n, 0] = rows
            for d in range(1, num_cols):
                self.coef(d).start()

        def ready(self, q):
            for c in range(2):
                if q == 0 and c == 1:
                    continue
                owner = partner if q == 0 else at_chip(q) * 2 + c
                arrived = self.coef(lax.rem(k - owner + num_cols, num_cols))
                arrived.wait_recv()

        def sent(self):
            for d in range(1, num_cols):
                pending.append(self.coef(d))

    first = Gather(0, field_one, True)

    def look_up(i):
        unroll = 16

        def some(n, _):
            base = n * unroll
            line = i * parts + base // 128
            lane = lax.rem(base, 128)
            for u in range(unroll):
                row = ids_smem[line, lane + u]
                looked_ref[pl.ds(base + u, 1), :] = wide_ref[pl.ds(row, 1), :]
            return 0

        lax.fori_loop(0, width // unroll, some, 0)
        first.field[k, i + 1] = looked_ref[...].astype(BF16)

    look_up(0)
    pl.semaphore_wait(barrier, num_cols - 1 + 2)
    if rounds > 0:
        tell_known(0)

    def open_gather(gather):
        for i, j in ((0, 3), (1, 2), (3, 0)):
            gather.own_right(i)
            gather.own_left(j)
        for i in (0, 3, 1, 2):
            gather.own(i)

    def pass_first(gather):
        gather.from_left(0)
        gather.from_right(3)
        gather.own_right(2)
        gather.own_left(1)

    inner, outer, every = (1, 2), (0, 3), (0, 1, 2, 3)

    first.own_right(0)
    first.halo_out(0, k, 0)
    first.own(0)
    look_up(3)
    first.own_left(3)
    first.halo_out(0, k, 3)
    first.own(3)
    look_up(1)
    first.own_right(1)
    first.own(1)
    look_up(2)
    first.own_left(2)
    first.own(2)
    first.own_right(3)
    first.own_left(0)
    pass_first(first)
    first.halo_in(0)
    meet(0)
    first.from_left(1)
    first.from_right(2)
    lay_tokens()
    first.rest(0)
    loads[1].wait()
    convolve(field_one, True, conv_one_ref, 0, every, False)
    first.from_left(3)
    first.from_right(0)
    first.from_far(0)
    first.from_far(3)
    meet(1)
    first.from_left(2)
    first.from_right(1)
    first.halo_in(1)
    first.halo_in(2)
    first.rest_rows(1, every)
    convolve(field_one, True, conv_one_ref, 1, inner)
    first.from_far(1)
    first.from_far(2)
    first.rest_rows(2, every)
    convolve(field_one, True, conv_one_ref, 2, inner)
    first.halo_in(3)
    meet(2)
    first.rest_halo(1)
    convolve(field_one, True, conv_one_ref, 1, outer)
    first.rest_halo(2)
    convolve(field_one, True, conv_one_ref, 2, outer)
    first.rest(3)
    convolve(field_one, True, conv_one_ref, 3, every)

    second = Gather(1, field_two, True)
    norm_one = Norm(0, gain_one_ref, bias_one_ref)
    for i in (0, 3, 1, 2):
        norm_one.row(i, second)
    open_gather(second)
    meet(3)
    norm_one.tell()
    second.halo_out(0, k, 0)
    second.halo_out(0, k, 3)
    pass_first(second)
    second.halo_in(0)
    norm_one.settle()
    second.from_left(1)
    second.from_right(2)
    second.from_left(3)
    second.from_right(0)
    second.from_far(0)
    second.from_far(3)
    second.rest(0)
    loads[2].wait()
    norm_one.ready(0)
    slots = range(height + 2)
    normalise(second, 0, slots)
    convolve(hidden_ref, False, conv_two_ref, 0, every, False)
    second.from_left(2)
    second.from_right(1)
    second.halo_in(1)
    second.halo_in(2)
    second.from_far(1)
    second.from_far(2)
    norm_one.ready(1)
    second.rest(1)
    normalise(second, 1, slots)
    second.halo_in(3)
    norm_one.ready(2)
    second.rest(2)
    normalise(second, 2, slots)
    convolve(hidden_ref, False, conv_two_ref, 1, every)
    norm_one.ready(3)
    second.rest(3)
    normalise(second, 3, slots)
    convolve(hidden_ref, False, conv_two_ref, 2, every)
    convolve(hidden_ref, False, conv_two_ref, 3, every)
    norm_one.sent()

    third = Gather(2, field_three, False)
    norm_two = Norm(1, gain_two_ref, bias_two_ref)
    for i in (0, 3, 1, 2):
        norm_two.row(i, third)
    open_gather(third)
    norm_two.tell()
    pass_first(third)
    norm_two.settle()
    third.from_left(1)
    third.from_right(2)
    scale_two = coef_all[1, 0, 0:1, :]
    shift_two = coef_all[1, 0, 2:3, :]
    for i in range(height):
        v = conv_ref[i * width : (i + 1) * width, :] * scale_two + shift_two
        features_ref[i] = (first.field[k, i + 1].astype(F32) + v).astype(BF16)

    vocab_here = head_hbm.shape[1]
    tiles = vocab_here // 128

    def all_features(i, to):
        for p in range(num_cols):
            d = lax.rem(k - p + num_cols, num_cols)
            v = third.field[p, i].astype(F32) * coef_all[1, d, 0:1, :] + coef_all[1, d, 2:3, :]
            v = first.field[p, i + 1].astype(F32) + v
            rows_ref[to, :, p * lanes : (p + 1) * lanes] = v.astype(BF16)

    def row_logits(to):
        logits_ref[to] = jnp.dot(rows_ref[to], head_ref[...], preferred_element_type=F32)

    def row_totals(i, to):
        most = logits_ref[to, :, 0:128]
        for t in range(1, tiles):
            most = jnp.maximum(most, logits_ref[to, :, 128 * t : 128 * t + 128])
        top = jnp.max(most, axis=1, keepdims=True)
        token = tokens_ref[i]
        lane = lax.broadcasted_iota(jnp.int32, (width, 128), 1)
        summed = jnp.zeros((width, 128), F32)
        picked = jnp.zeros((width, 128), F32)
        for t in range(tiles):
            part = logits_ref[to, :, 128 * t : 128 * t + 128]
            summed = summed + jnp.exp(part - top)
            ids = (lane + (k * vocab_here + 128 * t)).astype(F32)
            picked = picked + jnp.where(ids == token, part, 0.0)
        top_row = jnp.max(most.T, axis=0, keepdims=True)
        sum_row = jnp.sum(summed.T, axis=0, keepdims=True)
        pick_row = jnp.sum(picked.T, axis=0, keepdims=True)
        for n, row in enumerate((top_row, sum_row, pick_row)):
            for b in range(parts):
                last_send[b, n, i : i + 1, :] = row[:, 128 * b : 128 * b + 128]

    third.from_left(3)
    third.from_right(0)
    third.from_far(0)
    third.from_far(3)
    third.from_left(2)
    third.from_right(1)
    for q in range(4):
        third.rest_rows(q, (0, 3))
    loads[3].wait()
    for q in range(4):
        norm_two.ready(q)
    norm_two.sent()
    all_features(0, 0)
    row_logits(0)
    all_features(3, 1)
    third.from_far(1)
    third.from_far(2)
    row_logits(1)
    row_totals(0, 0)
    for q in range(4):
        third.rest_rows(q, (1, 2))
    all_features(1, 0)
    row_logits(0)
    row_totals(3, 1)
    all_features(2, 1)
    row_logits(1)
    row_totals(1, 0)
    row_totals(2, 1)

    per_block = num_cols // parts

    def exchange(d):
        to = lax.rem(k + d, num_cols)
        return pltpu.make_async_remote_copy(
            src_ref=last_send.at[to // per_block],
            dst_ref=last_all.at[d],
            send_sem=last_send_sems.at[d],
            recv_sem=last_recv_sems.at[d],
            device_id={"cols": to},
            device_id_type=MESH,
        )

    for d in range(1, num_cols):
        exchange(d).start()
    last_all[0] = last_send[k // per_block]
    for d in range(1, num_cols):
        exchange(d).wait_recv()
    totals_ref[...] = last_all[...]

    for copy in pending:
        copy.wait_send()
    for d in range(1, num_cols):
        exchange(d).wait_send()


def finish(num_cols, made_ref, last_all, features_ref, logp_ref):
    features_ref[...] = made_ref[...]
    per_block = num_cols // (made_ref.shape[1] // 128)
    mine = made_ref.shape[1] // num_cols
    top = last_all[0, 0]
    for d in range(1, num_cols):
        top = jnp.maximum(top, last_all[d, 0])
    summed = jnp.zeros_like(top)
    picked = jnp.zeros_like(top)
    for d in range(num_cols):
        summed = summed + last_all[d, 1] * jnp.exp(last_all[d, 0] - top)
        picked = picked + last_all[d, 2]
    logp = picked - top - jnp.log(summed)
    place = lax.rem(lax.axis_index("cols"), per_block)
    out = logp[:, 0:mine]
    for b in range(1, per_block):
        out = jnp.where(place == b, logp[:, mine * b : mine * b + mine], out)
    logp_ref[...] = out


def local(
    token_ids,
    keep_mask,
    remask_order,
    embed_table,
    mask_embed,
    conv_one,
    gain_one,
    bias_one,
    conv_two,
    gain_two,
    bias_two,
    head_weight,
):
    num_rows, num_cols = lax.axis_size("rows"), lax.axis_size("cols")
    height, width = token_ids.shape
    vocab, lanes = embed_table.shape
    lines = height * width // 128
    in_vmem = pl.BlockSpec(memory_space=pltpu.VMEM)
    anywhere = pl.BlockSpec(memory_space=pl.ANY)
    made, totals = pl.pallas_call(
        functools.partial(kernel, num_rows, num_cols),
        name="denoise",
        out_shape=(
            jax.ShapeDtypeStruct((height, width, lanes), BF16),
            jax.ShapeDtypeStruct((num_cols, 3, height, 128), F32),
        ),
        in_specs=[
            in_vmem,
            in_vmem,
            in_vmem,
            anywhere,
            in_vmem,
            anywhere,
            in_vmem,
            in_vmem,
            anywhere,
            in_vmem,
            in_vmem,
            anywhere,
        ],
        out_specs=(in_vmem, in_vmem),
        scratch_shapes=[
            pltpu.VMEM((vocab, lanes), BF16),
            pltpu.VMEM((vocab + 8, lanes), F32),
            pltpu.VMEM(conv_one.shape, BF16),
            pltpu.VMEM(conv_two.shape, BF16),
            pltpu.VMEM(head_weight.shape, BF16),
            pltpu.VMEM((lines, 128), jnp.int32),
            pltpu.SMEM((lines, 128), jnp.int32),
            pltpu.VMEM((height, width, 128), F32),
            pltpu.VMEM((width, lanes), F32),
            pltpu.VMEM((num_cols, height + 2, width, lanes), BF16),
            pltpu.VMEM((num_cols, height + 2, width, lanes), BF16),
            pltpu.VMEM((num_cols, height, width, lanes), BF16),
            pltpu.VMEM((height * width, 3 * lanes), F32),
            pltpu.VMEM((height * width, lanes), F32),
            pltpu.VMEM((2, 4, lanes), F32),
            pltpu.VMEM((2, num_rows, 4, lanes), F32),
            pltpu.VMEM((2, 4, lanes), F32),
            pltpu.VMEM((2, num_cols, 4, lanes), F32),
            pltpu.VMEM((num_cols, height + 2, width, lanes), BF16),
            pltpu.VMEM((2, width, num_cols * lanes), BF16),
            pltpu.VMEM((2, width, head_weight.shape[1]), F32),
            pltpu.VMEM((width // 128, 3, height, 128), F32),
            pltpu.VMEM((num_cols, 3, height, 128), F32),
            pltpu.SemaphoreType.DMA((5,)),
            pltpu.SemaphoreType.DMA((3, 11, 4)),
            pltpu.SemaphoreType.DMA((3, 11, 4)),
            pltpu.SemaphoreType.DMA((2,)),
            pltpu.SemaphoreType.DMA((2,)),
            pltpu.SemaphoreType.DMA((2, num_cols)),
            pltpu.SemaphoreType.DMA((2, num_cols)),
            pltpu.SemaphoreType.DMA((num_cols,)),
            pltpu.SemaphoreType.DMA((num_cols,)),
            pltpu.SemaphoreType.REGULAR((8,)),
        ],
        compiler_params=pltpu.CompilerParams(
            collective_id=0, has_side_effects=True, vmem_limit_bytes=60 * 1024 * 1024
        ),
    )(
        token_ids,
        keep_mask,
        remask_order.reshape(lines, 128),
        embed_table,
        mask_embed.reshape(1, lanes),
        conv_one,
        gain_one.reshape(1, lanes),
        bias_one.reshape(1, lanes),
        conv_two,
        gain_two.reshape(1, lanes),
        bias_two.reshape(1, lanes),
        head_weight,
    )
    return pl.pallas_call(
        functools.partial(finish, num_cols),
        name="finish",
        out_shape=(
            jax.ShapeDtypeStruct((height, width, lanes), BF16),
            jax.ShapeDtypeStruct((height, width // num_cols), F32),
        ),
        in_specs=[in_vmem, in_vmem],
        out_specs=(in_vmem, in_vmem),
    )(made, totals)


def solution(mesh):
    in_specs = (
        P("rows", None),
        P("rows", None),
        P("rows"),
        P(None, "cols"),
        P("cols"),
        P(None, None, None, "cols"),
        P("cols"),
        P("cols"),
        P(None, None, None, "cols"),
        P("cols"),
        P("cols"),
        P(None, "cols"),
    )
    out_specs = (P("rows", None, "cols"), P("rows", "cols"))
    return jax.shard_map(local, mesh=mesh, in_specs=in_specs, out_specs=out_specs, check_vma=False)
```

```python
import functools

import jax
import jax.numpy as jnp
from jax import lax
from jax.experimental import pallas as pl
from jax.experimental.pallas import tpu as pltpu
from jax.sharding import PartitionSpec as P

GROUP_WIDTH = 32
MESH = pl.DeviceIdType.MESH
F32 = jnp.float32
BF16 = jnp.bfloat16
XP, XM, OWN, FROM_P, FROM_M, FAR, FWD, UP, DOWN, UPF, DOWNF = range(11)


def group_sum(row):
    width = row.shape[1]
    a = lax.broadcasted_iota(jnp.int32, (width, width), 0) // GROUP_WIDTH
    b = lax.broadcasted_iota(jnp.int32, (width, width), 1) // GROUP_WIDTH
    ones = jnp.where(a == b, 1.0, 0.0).astype(F32)
    rows = jnp.broadcast_to(row, (8, width))
    return jnp.dot(
        rows, ones, preferred_element_type=F32, precision=lax.Precision.HIGHEST
    )[0:1]


def kernel(
    num_rows,
    num_cols,
    ids_hbm,
    keep_hbm,
    order_hbm,
    table_hbm,
    mask_hbm,
    conv_one_hbm,
    gain_one_hbm,
    bias_one_hbm,
    conv_two_hbm,
    gain_two_hbm,
    bias_two_hbm,
    head_hbm,
    features_hbm,
    totals_ref,
    ids_ref,
    keep_ref,
    order_ref,
    mask_ref,
    gain_one_ref,
    bias_one_ref,
    gain_two_ref,
    bias_two_ref,
    features_ref,
    table_ref,
    wide_ref,
    conv_one_ref,
    conv_two_ref,
    head_ref,
    ids_vmem,
    ids_smem,
    tokens_ref,
    looked_ref,
    field_one,
    field_two,
    field_three,
    total_ref,
    conv_ref,
    stat_send,
    stat_all,
    coef_send,
    coef_all,
    hidden_ref,
    rows_ref,
    early_ref,
    logits_ref,
    last_send,
    last_all,
    load_sems,
    send_sems,
    recv_sems,
    stat_send_sems,
    stat_recv_sems,
    coef_send_sems,
    coef_recv_sems,
    last_send_sems,
    last_recv_sems,
    known_sems,
):
    height, width = ids_hbm.shape
    vocab = table_hbm.shape[0]
    lanes = table_hbm.shape[1]
    channels = num_cols * lanes
    r = lax.axis_index("rows")
    k = lax.axis_index("cols")
    chips = num_cols // 2
    core = lax.rem(k, 2)
    chip = k // 2
    partner = k + 1 - 2 * core

    def piece(step, c):
        return lax.rem(chip + step, chips) * 2 + c

    right, left = piece(1, core), piece(chips - 1, core)
    above = lax.rem(r + num_rows - 1, num_rows)
    below = lax.rem(r + 1, num_rows)

    chunks = 4
    deep = vocab // chunks
    moves = [
        (ids_hbm, ids_ref),
        (keep_hbm, keep_ref),
        (order_hbm, order_ref),
        (mask_hbm, mask_ref),
    ]
    moves += [(table_hbm.at[pl.ds(n * deep, deep)], table_ref.at[pl.ds(n * deep, deep)]) for n in range(chunks)]
    moves += [
        (conv_one_hbm, conv_one_ref),
        (conv_two_hbm, conv_two_ref),
        (head_hbm, head_ref),
        (gain_one_hbm, gain_one_ref),
        (bias_one_hbm, bias_one_ref),
        (gain_two_hbm, gain_two_ref),
        (bias_two_hbm, bias_two_ref),
    ]
    loads = [
        pltpu.make_async_copy(src, dst, load_sems.at[n]) for n, (src, dst) in enumerate(moves)
    ]
    lookup_loads, table_loads, late_loads = loads[:4], loads[4 : 4 + chunks], loads[4 + chunks :]
    for load in lookup_loads + table_loads:
        load.start()

    barrier = pltpu.get_barrier_semaphore()

    def greet(device):
        pl.semaphore_signal(barrier, inc=1, device_id=device, device_id_type=MESH)

    for d in range(1, num_cols):
        greet({"cols": lax.rem(k + d, num_cols)})
    greet({"rows": above})
    greet({"rows": below})

    def tell_known(m):
        far = 2**m
        for to in (lax.rem(r + far, num_rows), lax.rem(r + num_rows - far, num_rows)):
            pl.semaphore_signal(
                known_sems.at[m], inc=1, device_id={"rows": to}, device_id_type=MESH
            )

    rounds = max(num_rows.bit_length() - 2, 0)

    def meet(m):
        if m < rounds:
            pl.semaphore_wait(known_sems.at[m], 2)
            if m + 1 < rounds:
                tell_known(m + 1)

    for load in lookup_loads:
        load.wait()
    half = height * width * num_rows // 2
    parts = width // 128
    for i in range(height):
        for j in range(parts):
            at = (slice(i, i + 1), slice(128 * j, 128 * j + 128))
            n = i * parts + j
            visible = (keep_ref[at] == 1) | (order_ref[n : n + 1, :] >= half)
            ids_vmem[n : n + 1, :] = jnp.where(visible, ids_ref[at], vocab)
    to_smem = pltpu.make_async_copy(ids_vmem, ids_smem, load_sems.at[len(moves)])
    to_smem.start()
    wide_ref[vocab : vocab + 8, :] = jnp.broadcast_to(mask_ref[...].astype(F32), (8, lanes))

    def lay_tokens():
        for i in range(height):
            row = ids_ref[i : i + 1, :].astype(F32)
            tokens_ref[i] = jnp.broadcast_to(row, (128, width)).T

    step_rows = 512
    for n in range(chunks):
        table_loads[n].wait()

        def widen(m, _, n=n):
            at = pl.ds(pl.multiple_of(n * deep + m * step_rows, step_rows), step_rows)
            wide_ref[at, :] = table_ref[at, :].astype(F32)
            return 0

        lax.fori_loop(0, deep // step_rows, widen, 0)
    for load in late_loads:
        load.start()
    to_smem.wait()

    pending = []

    class Gather:
        def __init__(self, n, field, halo):
            self.n, self.field, self.halo = n, field, halo
            self.off = 1 if halo else 0

        def copy(self, kind, slot, owner, row, device, to_row=None):
            to_row = row if to_row is None else to_row
            return pltpu.make_async_remote_copy(
                src_ref=self.field.at[owner, row],
                dst_ref=self.field.at[owner, to_row],
                send_sem=send_sems.at[self.n, kind, slot],
                recv_sem=recv_sems.at[self.n, kind, slot],
                device_id=device,
                device_id_type=MESH,
            )

        def send(self, *args, **kw):
            c = self.copy(*args, **kw)
            c.start()
            pending.append(c)

        def wait(self, kind, slot, owner, row):
            self.copy(kind, slot, owner, row, {"cols": partner}).wait_recv()

        def halo_out(self, q, owner, i):
            if not self.halo:
                return
            if i == 0:
                self.send(UP, q, owner, 1, {"rows": above}, to_row=height + 1)
            if i == height - 1:
                self.send(DOWN, q, owner, height, {"rows": below}, to_row=0)

        def own(self, i):
            self.send(OWN, i, k, i + self.off, {"cols": partner})

        def own_right(self, i):
            self.send(XP, i, k, i + self.off, {"cols": right})

        def own_left(self, i):
            self.send(XM, i, k, i + self.off, {"cols": left})

        def from_left(self, i):
            row, owner = i + self.off, left
            self.wait(XP, i, owner, row)
            if i in (0, 1):
                self.send(FWD, i, owner, row, {"cols": right})
            self.halo_out(1, owner, i)
            self.send(FROM_P, i, owner, row, {"cols": partner})

        def from_right(self, i):
            row, owner = i + self.off, right
            self.wait(XM, i, owner, row)
            if i in (2, 3):
                self.send(FWD, i, owner, row, {"cols": left})
            self.halo_out(2, owner, i)
            self.send(FROM_M, i, owner, row, {"cols": partner})

        def from_far(self, i):
            row, owner = i + self.off, piece(2, core)
            self.wait(FWD, i, owner, row)
            self.halo_out(3, owner, i)
            self.send(FAR, i, owner, row, {"cols": partner})

        def owner_of(self, q, c):
            return piece((0, chips - 1, 1, 2)[q], c)

        def halo_in(self, q):
            owner = self.owner_of(q, core)
            self.wait(UP, q, owner, height + 1)
            self.send(UPF, q, owner, height + 1, {"cols": partner})
            self.wait(DOWN, q, owner, 0)
            self.send(DOWNF, q, owner, 0, {"cols": partner})

        def rest_rows(self, q, rows):
            owner = self.owner_of(q, 1 - core)
            for i in rows:
                self.wait((OWN, FROM_P, FROM_M, FAR)[q], i, owner, i + self.off)

        def rest_halo(self, q):
            owner = self.owner_of(q, 1 - core)
            self.wait(UPF, q, owner, height + 1)
            self.wait(DOWNF, q, owner, 0)

        def rest(self, q):
            self.rest_rows(q, range(height))
            self.rest_halo(q)

    def at_chip(q):
        return lax.rem(chip + (0, chips - 1, 1, 2)[q], chips)

    def normalise(gather, q, slots):
        for c in range(2):
            owner = at_chip(q) * 2 + c
            d = lax.rem(k - owner + num_cols, num_cols)
            scale = coef_all[0, d, 0:1, :]
            for slot in slots:
                which = 1 + jnp.where(slot > 0, 1, 0) + jnp.where(slot > height, 1, 0)
                shift = coef_all[0, d, pl.ds(which, 1), :]
                inside = jnp.logical_and(
                    jnp.logical_or(r > 0, slot > 0),
                    jnp.logical_or(r < num_rows - 1, slot <= height),
                )
                v = gather.field[owner, slot].astype(F32) * (0.5 * scale) + 0.5 * shift
                v = v + v * jnp.tanh(v)
                hidden_ref[owner, slot] = jnp.where(inside, v, 0.0).astype(BF16)

    def convolve(field, masked, weight_ref, q, outs, started=True):
        at = at_chip(q)
        rows = pl.ds(pl.multiple_of(at * 2 * lanes, 2 * lanes), 2 * lanes)
        weights = jnp.concatenate(
            [
                jnp.concatenate([weight_ref[a, b, rows, :] for b in range(3)], axis=1)
                for a in range(3)
            ],
            axis=0,
        )
        columns = []
        for a in range(3):
            for p in (at * 2, at * 2 + 1):
                tiles = []
                for i in outs:
                    tile = field[p, i + a]
                    if masked and i + a == 0:
                        tile = jnp.where(r > 0, tile, jnp.zeros_like(tile))
                    if masked and i + a == height + 1:
                        tile = jnp.where(r < num_rows - 1, tile, jnp.zeros_like(tile))
                    tiles.append(tile)
                columns.append(jnp.concatenate(tiles, axis=0))
        product = jnp.dot(
            jnp.concatenate(columns, axis=1), weights, preferred_element_type=F32
        )
        for n, i in enumerate(outs):
            here = slice(i * width, (i + 1) * width)
            part = product[n * width : (n + 1) * width]
            if started:
                total_ref[here, :] += part
            else:
                total_ref[here, :] = part

    def shifted_row(i):
        index = lax.broadcasted_iota(jnp.int32, (width, lanes), 0)
        at = slice(i * width, (i + 1) * width)
        before = pltpu.roll(total_ref[at, 0:lanes], 1, axis=0)
        after = pltpu.roll(total_ref[at, 2 * lanes : 3 * lanes], width - 1, axis=0)
        return (
            jnp.where(index == 0, 0.0, before)
            + total_ref[at, lanes : 2 * lanes]
            + jnp.where(index == width - 1, 0.0, after)
        )

    positions = height * width
    count = positions * GROUP_WIDTH

    deep_z = min(8, num_rows)
    deep_y = num_rows // deep_z

    def row_at(d):
        y = lax.rem(r // deep_z + d // deep_z, deep_y)
        return y * deep_z + lax.rem(lax.rem(r, deep_z) + d % deep_z, deep_z)

    def hops(d):
        y, z = d // deep_z, d % deep_z
        return min(y, deep_y - y) + min(z, deep_z - z)

    far_first = sorted(range(1, num_rows), key=hops, reverse=True)
    at_start = jnp.where(lax.rem(r, deep_z) == 0, 1, 0)
    at_end = jnp.where(lax.rem(r, deep_z) == deep_z - 1, 1, 0)
    slot_above = lax.rem(1 + deep_z * at_start, num_rows)
    slot_below = deep_z - 1 + deep_z * (deep_y - 1) * at_end

    class Norm:
        def __init__(self, n, gain, bias):
            self.n, self.gain, self.bias = n, gain, bias
            self.centre = self.sums = self.squares = None

        def row(self, i, gather):
            values = shifted_row(i)
            if self.centre is None:
                self.centre = jnp.sum(values, axis=0, keepdims=True) / width
            values = values - self.centre
            gather.field[k, i + gather.off] = values.astype(BF16)
            conv_ref[i * width : (i + 1) * width, :] = values
            total = jnp.sum(values, axis=0, keepdims=True)
            square = jnp.sum(values * values, axis=0, keepdims=True)
            self.sums = total if self.sums is None else self.sums + total
            self.squares = square if self.squares is None else self.squares + square

        def tell(self):
            n = self.n
            mean = group_sum(self.sums + positions * self.centre) / count
            off = self.centre - mean
            square = group_sum(self.squares + 2 * off * self.sums + positions * off * off)
            both = jnp.concatenate([mean, square, self.centre, self.centre], axis=0)
            stat_send[n] = both
            stat_all[n, 0] = both

            for d in far_first:
                pltpu.make_async_remote_copy(
                    src_ref=stat_send.at[n],
                    dst_ref=stat_all.at[n, d],
                    send_sem=stat_send_sems.at[n],
                    recv_sem=stat_recv_sems.at[n],
                    device_id={"rows": row_at(d)},
                    device_id_type=MESH,
                ).start()

        def coef(self, d):
            n = self.n
            return pltpu.make_async_remote_copy(
                src_ref=coef_send.at[n],
                dst_ref=coef_all.at[n, d],
                send_sem=coef_send_sems.at[n, d],
                recv_sem=coef_recv_sems.at[n, d],
                device_id={"cols": lax.rem(k + d, num_cols)},
                device_id_type=MESH,
            )

        def settle(self):
            n = self.n
            everything = stat_all.at[n, pl.ds(1, num_rows - 1)]
            arrived = pltpu.make_async_remote_copy(
                src_ref=everything,
                dst_ref=everything,
                send_sem=stat_send_sems.at[n],
                recv_sem=stat_recv_sems.at[n],
                device_id={"rows": above},
                device_id_type=MESH,
            )
            arrived.wait_recv()
            pending.append(arrived)
            means = stat_all[n, :, 0, :]
            mean = jnp.sum(means, axis=0, keepdims=True) / num_rows
            spread = means - mean
            square = jnp.sum(stat_all[n, :, 1, :], axis=0, keepdims=True)
            square = square + count * jnp.sum(spread * spread, axis=0, keepdims=True)
            variance = square / (count * num_rows)
            scale = self.gain[...] / jnp.sqrt(variance + 1e-5)
            centres = [stat_all[n, d, 2:3, :] for d in (slot_above, 0, slot_below)]
            shifts = [(c - mean) * scale + self.bias[...] for c in centres]
            rows = jnp.concatenate([scale] + shifts, axis=0)
            coef_send[n] = rows
            coef_all[n, 0] = rows
            for d in range(1, num_cols):
                self.coef(d).start()

        def ready(self, q):
            for c in range(2):
                if q == 0 and c == 1:
                    continue
                owner = partner if q == 0 else at_chip(q) * 2 + c
                arrived = self.coef(lax.rem(k - owner + num_cols, num_cols))
                arrived.wait_recv()

        def sent(self):
            for d in range(1, num_cols):
                pending.append(self.coef(d))

    first = Gather(0, field_one, True)

    def look_up(i):
        unroll = 64

        def some(n, _):
            base = n * unroll
            line = i * parts + base // 128
            lane = lax.rem(base, 128)
            for u in range(unroll):
                row = ids_smem[line, lane + u]
                looked_ref[pl.ds(base + u, 1), :] = wide_ref[pl.ds(row, 1), :]
            return 0

        lax.fori_loop(0, width // unroll, some, 0)
        first.field[k, i + 1] = looked_ref[...].astype(BF16)

    look_up(0)
    pl.semaphore_wait(barrier, num_cols - 1 + 2)
    if rounds > 0:
        tell_known(0)

    def open_gather(gather):
        for i, j in ((0, 3), (1, 2), (3, 0)):
            gather.own_right(i)
            gather.own_left(j)
        for i in (0, 3, 1, 2):
            gather.own(i)

    def pass_first(gather):
        gather.from_left(0)
        gather.from_right(3)
        gather.own_right(2)
        gather.own_left(1)

    inner, outer, every = (1, 2), (0, 3), (0, 1, 2, 3)

    first.own_right(0)
    first.halo_out(0, k, 0)
    first.own(0)
    look_up(3)
    first.own_left(3)
    first.halo_out(0, k, 3)
    first.own(3)
    look_up(1)
    first.own_right(1)
    first.own(1)
    look_up(2)
    first.own_left(2)
    first.own(2)
    first.own_right(3)
    first.own_left(0)
    pass_first(first)
    first.halo_in(0)
    meet(0)
    first.from_left(1)
    first.from_right(2)
    lay_tokens()
    first.rest(0)
    late_loads[0].wait()
    convolve(field_one, True, conv_one_ref, 0, every, False)
    first.from_left(3)
    first.from_right(0)
    first.from_far(0)
    first.from_far(3)
    meet(1)
    first.from_left(2)
    first.from_right(1)
    first.halo_in(1)
    first.halo_in(2)
    first.rest_rows(1, every)
    convolve(field_one, True, conv_one_ref, 1, inner)
    first.from_far(1)
    first.from_far(2)
    first.rest_rows(2, every)
    convolve(field_one, True, conv_one_ref, 2, inner)
    first.halo_in(3)
    meet(2)
    first.rest_halo(1)
    convolve(field_one, True, conv_one_ref, 1, outer)
    first.rest_halo(2)
    convolve(field_one, True, conv_one_ref, 2, outer)
    first.rest(3)
    convolve(field_one, True, conv_one_ref, 3, every)

    second = Gather(1, field_two, True)
    norm_one = Norm(0, gain_one_ref, bias_one_ref)
    for i in (0, 3, 1, 2):
        norm_one.row(i, second)
    open_gather(second)
    meet(3)
    norm_one.tell()
    second.halo_out(0, k, 0)
    second.halo_out(0, k, 3)
    pass_first(second)
    second.halo_in(0)
    second.from_left(3)
    second.from_right(0)
    late_loads[3].wait()
    late_loads[4].wait()
    norm_one.settle()
    second.from_left(1)
    second.from_right(2)
    second.from_far(0)
    second.from_far(3)
    second.rest(0)
    late_loads[1].wait()
    norm_one.ready(0)
    slots = range(height + 2)
    normalise(second, 0, slots)
    convolve(hidden_ref, False, conv_two_ref, 0, every, False)
    second.from_left(2)
    second.from_right(1)
    second.halo_in(1)
    second.halo_in(2)
    second.from_far(1)
    second.from_far(2)
    middle, ends = range(1, height + 1), (0, height + 1)
    norm_one.ready(1)
    second.rest_rows(1, every)
    normalise(second, 1, middle)
    norm_one.ready(2)
    second.rest_rows(2, every)
    convolve(hidden_ref, False, conv_two_ref, 1, inner)
    normalise(second, 2, middle)
    second.halo_in(3)
    second.rest_halo(1)
    convolve(hidden_ref, False, conv_two_ref, 2, inner)
    normalise(second, 1, ends)
    second.rest_halo(2)
    convolve(hidden_ref, False, conv_two_ref, 1, outer)
    normalise(second, 2, ends)
    norm_one.ready(3)
    second.rest(3)
    convolve(hidden_ref, False, conv_two_ref, 2, outer)
    normalise(second, 3, slots)
    convolve(hidden_ref, False, conv_two_ref, 3, every)
    norm_one.sent()

    third = Gather(2, field_three, False)
    norm_two = Norm(1, gain_two_ref, bias_two_ref)
    for i in (0, 3, 1, 2):
        norm_two.row(i, third)
    open_gather(third)
    norm_two.tell()
    pass_first(third)
    late_loads[5].wait()
    late_loads[6].wait()
    norm_two.settle()
    third.from_left(1)
    third.from_right(2)
    scale_two = coef_all[1, 0, 0:1, :]
    shift_two = coef_all[1, 0, 2:3, :]
    vocab_here = head_hbm.shape[1]
    tiles = vocab_here // 128

    def features_of(p, i):
        d = lax.rem(k - p + num_cols, num_cols)
        v = third.field[p, i].astype(F32) * coef_all[1, d, 0:1, :] + coef_all[1, d, 2:3, :]
        return (first.field[p, i + 1].astype(F32) + v).astype(BF16)

    def head_rows_of(q):
        at = at_chip(q)
        return head_ref[pl.ds(pl.multiple_of(at * 2 * lanes, 2 * lanes), 2 * lanes), :]

    def own_logits():
        for i in range(height):
            made = [features_of(at_chip(0) * 2 + c, i) for c in range(2)]
            early_ref[i] = jnp.dot(
                jnp.concatenate(made, axis=1), head_rows_of(0), preferred_element_type=F32
            )

    def all_features(i, to):
        for q in range(1, 4):
            for c in range(2):
                n = 2 * (q - 1) + c
                rows_ref[to, :, n * lanes : (n + 1) * lanes] = features_of(at_chip(q) * 2 + c, i)

    def row_logits(i, to):
        weights = jnp.concatenate([head_rows_of(q) for q in range(1, 4)], axis=0)
        logits_ref[to] = early_ref[i] + jnp.dot(
            rows_ref[to], weights, preferred_element_type=F32
        )

    def row_totals(i, to):
        most = logits_ref[to, :, 0:128]
        for t in range(1, tiles):
            most = jnp.maximum(most, logits_ref[to, :, 128 * t : 128 * t + 128])
        top = jnp.max(most, axis=1, keepdims=True)
        token = tokens_ref[i]
        lane = lax.broadcasted_iota(jnp.int32, (width, 128), 1)
        summed = jnp.zeros((width, 128), F32)
        picked = jnp.zeros((width, 128), F32)
        for t in range(tiles):
            part = logits_ref[to, :, 128 * t : 128 * t + 128]
            summed = summed + jnp.exp(part - top)
            ids = (lane + (k * vocab_here + 128 * t)).astype(F32)
            picked = picked + jnp.where(ids == token, part, 0.0)
        top_row = jnp.max(most.T, axis=0, keepdims=True)
        sum_row = jnp.sum(summed.T, axis=0, keepdims=True)
        pick_row = jnp.sum(picked.T, axis=0, keepdims=True)
        for n, row in enumerate((top_row, sum_row, pick_row)):
            for b in range(parts):
                last_send[b, n, i : i + 1, :] = row[:, 128 * b : 128 * b + 128]

    third.from_left(3)
    third.from_right(0)
    third.from_far(0)
    third.from_far(3)
    for i in range(height):
        v = conv_ref[i * width : (i + 1) * width, :] * scale_two + shift_two
        features_ref[i] = (first.field[k, i + 1].astype(F32) + v).astype(BF16)
    features_out = pltpu.make_async_copy(features_ref, features_hbm, load_sems.at[16])
    features_out.start()
    third.rest_rows(0, every)
    late_loads[2].wait()
    norm_two.ready(0)
    own_logits()
    third.from_left(2)
    third.from_right(1)
    for q in range(1, 4):
        third.rest_rows(q, (0, 3))
        norm_two.ready(q)
    norm_two.sent()
    all_features(0, 0)
    row_logits(0, 0)
    all_features(3, 1)
    third.from_far(1)
    third.from_far(2)
    row_logits(3, 1)
    row_totals(0, 0)
    for q in range(1, 4):
        third.rest_rows(q, (1, 2))
    all_features(1, 0)
    row_logits(1, 0)
    row_totals(3, 1)
    all_features(2, 1)
    row_logits(2, 1)
    row_totals(1, 0)
    row_totals(2, 1)

    per_block = num_cols // parts

    def exchange(d):
        to = lax.rem(k + d, num_cols)
        return pltpu.make_async_remote_copy(
            src_ref=last_send.at[to // per_block],
            dst_ref=last_all.at[d],
            send_sem=last_send_sems.at[d],
            recv_sem=last_recv_sems.at[d],
            device_id={"cols": to},
            device_id_type=MESH,
        )

    for d in range(1, num_cols):
        exchange(d).start()
    last_all[0] = last_send[k // per_block]
    for d in range(1, num_cols):
        exchange(d).wait_recv()
    totals_ref[...] = last_all[...]
    features_out.wait()

    for copy in pending:
        copy.wait_send()
    for d in range(1, num_cols):
        exchange(d).wait_send()


def finish(num_cols, made_ref, last_all, features_ref, logp_ref):
    features_ref[...] = made_ref[...]
    per_block = num_cols // (made_ref.shape[1] // 128)
    mine = made_ref.shape[1] // num_cols
    top = last_all[0, 0]
    for d in range(1, num_cols):
        top = jnp.maximum(top, last_all[d, 0])
    summed = jnp.zeros_like(top)
    picked = jnp.zeros_like(top)
    for d in range(num_cols):
        summed = summed + last_all[d, 1] * jnp.exp(last_all[d, 0] - top)
        picked = picked + last_all[d, 2]
    logp = picked - top - jnp.log(summed)
    place = lax.rem(lax.axis_index("cols"), per_block)
    out = logp[:, 0:mine]
    for b in range(1, per_block):
        out = jnp.where(place == b, logp[:, mine * b : mine * b + mine], out)
    logp_ref[...] = out


def local(
    token_ids,
    keep_mask,
    remask_order,
    embed_table,
    mask_embed,
    conv_one,
    gain_one,
    bias_one,
    conv_two,
    gain_two,
    bias_two,
    head_weight,
):
    num_rows, num_cols = lax.axis_size("rows"), lax.axis_size("cols")
    height, width = token_ids.shape
    vocab, lanes = embed_table.shape
    lines = height * width // 128
    in_vmem = pl.BlockSpec(memory_space=pltpu.VMEM)
    anywhere = pl.BlockSpec(memory_space=pl.ANY)
    made, totals = pl.pallas_call(
        functools.partial(kernel, num_rows, num_cols),
        name="denoise",
        out_shape=(
            jax.ShapeDtypeStruct((height, width, lanes), BF16),
            jax.ShapeDtypeStruct((num_cols, 3, height, 128), F32),
        ),
        in_specs=[anywhere] * 12,
        out_specs=(anywhere, in_vmem),
        scratch_shapes=[
            pltpu.VMEM((height, width), jnp.int32),
            pltpu.VMEM((height, width), jnp.int32),
            pltpu.VMEM((lines, 128), jnp.int32),
            pltpu.VMEM((1, lanes), BF16),
            pltpu.VMEM((1, lanes), F32),
            pltpu.VMEM((1, lanes), F32),
            pltpu.VMEM((1, lanes), F32),
            pltpu.VMEM((1, lanes), F32),
            pltpu.VMEM((height, width, lanes), BF16),
            pltpu.VMEM((vocab, lanes), BF16),
            pltpu.VMEM((vocab + 8, lanes), F32),
            pltpu.VMEM(conv_one.shape, BF16),
            pltpu.VMEM(conv_two.shape, BF16),
            pltpu.VMEM(head_weight.shape, BF16),
            pltpu.VMEM((lines, 128), jnp.int32),
            pltpu.SMEM((lines, 128), jnp.int32),
            pltpu.VMEM((height, width, 128), F32),
            pltpu.VMEM((width, lanes), F32),
            pltpu.VMEM((num_cols, height + 2, width, lanes), BF16),
            pltpu.VMEM((num_cols, height + 2, width, lanes), BF16),
            pltpu.VMEM((num_cols, height, width, lanes), BF16),
            pltpu.VMEM((height * width, 3 * lanes), F32),
            pltpu.VMEM((height * width, lanes), F32),
            pltpu.VMEM((2, 4, lanes), F32),
            pltpu.VMEM((2, num_rows, 4, lanes), F32),
            pltpu.VMEM((2, 4, lanes), F32),
            pltpu.VMEM((2, num_cols, 4, lanes), F32),
            pltpu.VMEM((num_cols, height + 2, width, lanes), BF16),
            pltpu.VMEM((2, width, (num_cols - 2) * lanes), BF16),
            pltpu.VMEM((height, width, head_weight.shape[1]), F32),
            pltpu.VMEM((2, width, head_weight.shape[1]), F32),
            pltpu.VMEM((width // 128, 3, height, 128), F32),
            pltpu.VMEM((num_cols, 3, height, 128), F32),
            pltpu.SemaphoreType.DMA((17,)),
            pltpu.SemaphoreType.DMA((3, 11, 4)),
            pltpu.SemaphoreType.DMA((3, 11, 4)),
            pltpu.SemaphoreType.DMA((2,)),
            pltpu.SemaphoreType.DMA((2,)),
            pltpu.SemaphoreType.DMA((2, num_cols)),
            pltpu.SemaphoreType.DMA((2, num_cols)),
            pltpu.SemaphoreType.DMA((num_cols,)),
            pltpu.SemaphoreType.DMA((num_cols,)),
            pltpu.SemaphoreType.REGULAR((8,)),
        ],
        compiler_params=pltpu.CompilerParams(
            collective_id=0, has_side_effects=True, vmem_limit_bytes=60 * 1024 * 1024
        ),
    )(
        token_ids,
        keep_mask,
        remask_order.reshape(lines, 128),
        embed_table,
        mask_embed.reshape(1, lanes),
        conv_one,
        gain_one.reshape(1, lanes),
        bias_one.reshape(1, lanes),
        conv_two,
        gain_two.reshape(1, lanes),
        bias_two.reshape(1, lanes),
        head_weight,
    )
    return pl.pallas_call(
        functools.partial(finish, num_cols),
        name="finish",
        out_shape=(
            jax.ShapeDtypeStruct((height, width, lanes), BF16),
            jax.ShapeDtypeStruct((height, width // num_cols), F32),
        ),
        in_specs=[in_vmem, in_vmem],
        out_specs=(in_vmem, in_vmem),
    )(made, totals)


def solution(mesh):
    in_specs = (
        P("rows", None),
        P("rows", None),
        P("rows"),
        P(None, "cols"),
        P("cols"),
        P(None, None, None, "cols"),
        P("cols"),
        P("cols"),
        P(None, None, None, "cols"),
        P("cols"),
        P("cols"),
        P(None, "cols"),
    )
    out_specs = (P("rows", None, "cols"), P("rows", "cols"))
    return jax.shard_map(local, mesh=mesh, in_specs=in_specs, out_specs=out_specs, check_vma=False)
```

```python
import functools

import jax
import jax.numpy as jnp
from jax import lax
from jax.experimental import pallas as pl
from jax.experimental.pallas import tpu as pltpu
from jax.sharding import PartitionSpec as P

GROUP_WIDTH = 32
MESH = pl.DeviceIdType.MESH
F32 = jnp.float32
BF16 = jnp.bfloat16
XP, XM, OWN, FROM_P, FROM_M, FAR, FWD, UP, DOWN, UPF, DOWNF = range(11)


def group_sum(row):
    width = row.shape[1]
    a = lax.broadcasted_iota(jnp.int32, (width, width), 0) // GROUP_WIDTH
    b = lax.broadcasted_iota(jnp.int32, (width, width), 1) // GROUP_WIDTH
    ones = jnp.where(a == b, 1.0, 0.0).astype(F32)
    rows = jnp.broadcast_to(row, (8, width))
    return jnp.dot(
        rows, ones, preferred_element_type=F32, precision=lax.Precision.HIGHEST
    )[0:1]


def kernel(
    num_rows,
    num_cols,
    ids_hbm,
    keep_hbm,
    order_hbm,
    table_hbm,
    mask_hbm,
    conv_one_hbm,
    gain_one_hbm,
    bias_one_hbm,
    conv_two_hbm,
    gain_two_hbm,
    bias_two_hbm,
    head_hbm,
    features_hbm,
    totals_ref,
    ids_ref,
    keep_ref,
    order_ref,
    mask_ref,
    gain_one_ref,
    bias_one_ref,
    gain_two_ref,
    bias_two_ref,
    features_ref,
    table_ref,
    wide_ref,
    conv_one_ref,
    conv_two_ref,
    head_ref,
    ids_vmem,
    ids_smem,
    tokens_ref,
    looked_ref,
    field_one,
    field_two,
    field_three,
    total_ref,
    conv_ref,
    stat_send,
    stat_all,
    coef_send,
    coef_all,
    hidden_ref,
    rows_ref,
    early_ref,
    logits_ref,
    last_send,
    last_all,
    load_sems,
    send_sems,
    recv_sems,
    stat_send_sems,
    stat_recv_sems,
    coef_send_sems,
    coef_recv_sems,
    last_send_sems,
    last_recv_sems,
    known_sems,
):
    height, width = ids_hbm.shape
    vocab = table_hbm.shape[0]
    lanes = table_hbm.shape[1]
    channels = num_cols * lanes
    r = lax.axis_index("rows")
    k = lax.axis_index("cols")
    chips = num_cols // 2
    core = lax.rem(k, 2)
    chip = k // 2
    partner = k + 1 - 2 * core

    def piece(step, c):
        return lax.rem(chip + step, chips) * 2 + c

    right, left = piece(1, core), piece(chips - 1, core)
    above = lax.rem(r + num_rows - 1, num_rows)
    below = lax.rem(r + 1, num_rows)

    chunks = 4
    deep = vocab // chunks
    moves = [
        (ids_hbm, ids_ref),
        (keep_hbm, keep_ref),
        (order_hbm, order_ref),
        (mask_hbm, mask_ref),
    ]
    moves += [(table_hbm.at[pl.ds(n * deep, deep)], table_ref.at[pl.ds(n * deep, deep)]) for n in range(chunks)]
    moves += [
        (conv_one_hbm, conv_one_ref),
        (conv_two_hbm, conv_two_ref),
        (head_hbm, head_ref),
        (gain_one_hbm, gain_one_ref),
        (bias_one_hbm, bias_one_ref),
        (gain_two_hbm, gain_two_ref),
        (bias_two_hbm, bias_two_ref),
    ]
    loads = [
        pltpu.make_async_copy(src, dst, load_sems.at[n]) for n, (src, dst) in enumerate(moves)
    ]
    lookup_loads, table_loads, late_loads = loads[:4], loads[4 : 4 + chunks], loads[4 + chunks :]
    for load in lookup_loads + table_loads:
        load.start()

    barrier = pltpu.get_barrier_semaphore()

    def greet(device):
        pl.semaphore_signal(barrier, inc=1, device_id=device, device_id_type=MESH)

    for d in range(1, num_cols):
        greet({"cols": lax.rem(k + d, num_cols)})
    greet({"rows": above})
    greet({"rows": below})

    def tell_known(m):
        far = 2**m
        for to in (lax.rem(r + far, num_rows), lax.rem(r + num_rows - far, num_rows)):
            pl.semaphore_signal(
                known_sems.at[m], inc=1, device_id={"rows": to}, device_id_type=MESH
            )

    rounds = max(num_rows.bit_length() - 2, 0)

    def meet(m):
        if m < rounds:
            pl.semaphore_wait(known_sems.at[m], 2)
            if m + 1 < rounds:
                tell_known(m + 1)

    for load in lookup_loads:
        load.wait()
    half = height * width * num_rows // 2
    parts = width // 128
    for i in range(height):
        for j in range(parts):
            at = (slice(i, i + 1), slice(128 * j, 128 * j + 128))
            n = i * parts + j
            visible = (keep_ref[at] == 1) | (order_ref[n : n + 1, :] >= half)
            ids_vmem[n : n + 1, :] = jnp.where(visible, ids_ref[at], vocab)
    to_smem = pltpu.make_async_copy(ids_vmem, ids_smem, load_sems.at[len(moves)])
    to_smem.start()
    wide_ref[vocab : vocab + 8, :] = jnp.broadcast_to(mask_ref[...].astype(F32), (8, lanes))

    def lay_tokens():
        for i in range(height):
            row = ids_ref[i : i + 1, :].astype(F32)
            tokens_ref[i] = jnp.broadcast_to(row, (128, width)).T

    step_rows = 512
    for n in range(chunks):
        table_loads[n].wait()

        def widen(m, _, n=n):
            at = pl.ds(pl.multiple_of(n * deep + m * step_rows, step_rows), step_rows)
            wide_ref[at, :] = table_ref[at, :].astype(F32)
            return 0

        lax.fori_loop(0, deep // step_rows, widen, 0)
    for load in late_loads:
        load.start()
    to_smem.wait()

    pending = []

    class Gather:
        def __init__(self, n, field, halo):
            self.n, self.field, self.halo = n, field, halo
            self.off = 1 if halo else 0

        def copy(self, kind, slot, owner, row, device, to_row=None):
            to_row = row if to_row is None else to_row
            return pltpu.make_async_remote_copy(
                src_ref=self.field.at[owner, row],
                dst_ref=self.field.at[owner, to_row],
                send_sem=send_sems.at[self.n, kind, slot],
                recv_sem=recv_sems.at[self.n, kind, slot],
                device_id=device,
                device_id_type=MESH,
            )

        def send(self, *args, **kw):
            c = self.copy(*args, **kw)
            c.start()
            pending.append(c)

        def wait(self, kind, slot, owner, row):
            self.copy(kind, slot, owner, row, {"cols": partner}).wait_recv()

        def halo_out(self, q, owner, i):
            if not self.halo:
                return
            if i == 0:
                self.send(UP, q, owner, 1, {"rows": above}, to_row=height + 1)
            if i == height - 1:
                self.send(DOWN, q, owner, height, {"rows": below}, to_row=0)

        def own(self, i):
            self.send(OWN, i, k, i + self.off, {"cols": partner})

        def own_right(self, i):
            self.send(XP, i, k, i + self.off, {"cols": right})

        def own_left(self, i):
            self.send(XM, i, k, i + self.off, {"cols": left})

        def from_left(self, i):
            row, owner = i + self.off, left
            self.wait(XP, i, owner, row)
            if i in (0, 1):
                self.send(FWD, i, owner, row, {"cols": right})
            self.halo_out(1, owner, i)
            self.send(FROM_P, i, owner, row, {"cols": partner})

        def from_right(self, i):
            row, owner = i + self.off, right
            self.wait(XM, i, owner, row)
            if i in (2, 3):
                self.send(FWD, i, owner, row, {"cols": left})
            self.halo_out(2, owner, i)
            self.send(FROM_M, i, owner, row, {"cols": partner})

        def from_far(self, i):
            row, owner = i + self.off, piece(2, core)
            self.wait(FWD, i, owner, row)
            self.halo_out(3, owner, i)
            self.send(FAR, i, owner, row, {"cols": partner})

        def owner_of(self, q, c):
            return piece((0, chips - 1, 1, 2)[q], c)

        def halo_in(self, q):
            owner = self.owner_of(q, core)
            self.wait(UP, q, owner, height + 1)
            self.send(UPF, q, owner, height + 1, {"cols": partner})
            self.wait(DOWN, q, owner, 0)
            self.send(DOWNF, q, owner, 0, {"cols": partner})

        def rest_rows(self, q, rows):
            owner = self.owner_of(q, 1 - core)
            for i in rows:
                self.wait((OWN, FROM_P, FROM_M, FAR)[q], i, owner, i + self.off)

        def rest_halo(self, q):
            owner = self.owner_of(q, 1 - core)
            self.wait(UPF, q, owner, height + 1)
            self.wait(DOWNF, q, owner, 0)

        def rest(self, q):
            self.rest_rows(q, range(height))
            self.rest_halo(q)

    def at_chip(q):
        return lax.rem(chip + (0, chips - 1, 1, 2)[q], chips)

    def normalise(gather, q, slots, cores=(0, 1)):
        for c in cores:
            owner = at_chip(q) * 2 + c
            d = lax.rem(k - owner + num_cols, num_cols)
            scale = coef_all[0, d, 0:1, :]
            for slot in slots:
                which = 1 + jnp.where(slot > 0, 1, 0) + jnp.where(slot > height, 1, 0)
                shift = coef_all[0, d, pl.ds(which, 1), :]
                inside = jnp.logical_and(
                    jnp.logical_or(r > 0, slot > 0),
                    jnp.logical_or(r < num_rows - 1, slot <= height),
                )
                v = gather.field[owner, slot].astype(F32) * (0.5 * scale) + 0.5 * shift
                v = v + v * jnp.tanh(v)
                hidden_ref[owner, slot] = jnp.where(inside, v, 0.0).astype(BF16)

    def convolve(field, masked, weight_ref, q, outs, started=True):
        at = at_chip(q)
        rows = pl.ds(pl.multiple_of(at * 2 * lanes, 2 * lanes), 2 * lanes)
        weights = jnp.concatenate(
            [
                jnp.concatenate([weight_ref[a, b, rows, :] for b in range(3)], axis=1)
                for a in range(3)
            ],
            axis=0,
        )
        columns = []
        for a in range(3):
            for p in (at * 2, at * 2 + 1):
                tiles = []
                for i in outs:
                    tile = field[p, i + a]
                    if masked and i + a == 0:
                        tile = jnp.where(r > 0, tile, jnp.zeros_like(tile))
                    if masked and i + a == height + 1:
                        tile = jnp.where(r < num_rows - 1, tile, jnp.zeros_like(tile))
                    tiles.append(tile)
                columns.append(jnp.concatenate(tiles, axis=0))
        product = jnp.dot(
            jnp.concatenate(columns, axis=1), weights, preferred_element_type=F32
        )
        for n, i in enumerate(outs):
            here = slice(i * width, (i + 1) * width)
            part = product[n * width : (n + 1) * width]
            if started:
                total_ref[here, :] += part
            else:
                total_ref[here, :] = part

    def shifted_row(i):
        index = lax.broadcasted_iota(jnp.int32, (width, lanes), 0)
        at = slice(i * width, (i + 1) * width)
        before = pltpu.roll(total_ref[at, 0:lanes], 1, axis=0)
        after = pltpu.roll(total_ref[at, 2 * lanes : 3 * lanes], width - 1, axis=0)
        return (
            jnp.where(index == 0, 0.0, before)
            + total_ref[at, lanes : 2 * lanes]
            + jnp.where(index == width - 1, 0.0, after)
        )

    positions = height * width
    count = positions * GROUP_WIDTH

    deep_z = min(8, num_rows)
    deep_y = num_rows // deep_z

    def row_at(d):
        y = lax.rem(r // deep_z + d // deep_z, deep_y)
        return y * deep_z + lax.rem(lax.rem(r, deep_z) + d % deep_z, deep_z)

    def hops(d):
        y, z = d // deep_z, d % deep_z
        return min(y, deep_y - y) + min(z, deep_z - z)

    far_first = sorted(range(1, num_rows), key=hops, reverse=True)
    at_start = jnp.where(lax.rem(r, deep_z) == 0, 1, 0)
    at_end = jnp.where(lax.rem(r, deep_z) == deep_z - 1, 1, 0)
    slot_above = lax.rem(1 + deep_z * at_start, num_rows)
    slot_below = deep_z - 1 + deep_z * (deep_y - 1) * at_end

    class Norm:
        def __init__(self, n, gain, bias):
            self.n, self.gain, self.bias = n, gain, bias
            self.centre = self.sums = self.squares = None

        def row(self, i, gather):
            values = shifted_row(i)
            if self.centre is None:
                self.centre = jnp.sum(values, axis=0, keepdims=True) / width
            values = values - self.centre
            gather.field[k, i + gather.off] = values.astype(BF16)
            conv_ref[i * width : (i + 1) * width, :] = values
            total = jnp.sum(values, axis=0, keepdims=True)
            square = jnp.sum(values * values, axis=0, keepdims=True)
            self.sums = total if self.sums is None else self.sums + total
            self.squares = square if self.squares is None else self.squares + square

        def tell(self):
            n = self.n
            mean = group_sum(self.sums + positions * self.centre) / count
            off = self.centre - mean
            square = group_sum(self.squares + 2 * off * self.sums + positions * off * off)
            both = jnp.concatenate([mean, square, self.centre, self.centre], axis=0)
            stat_send[n] = both
            stat_all[n, 0] = both

            for d in far_first:
                pltpu.make_async_remote_copy(
                    src_ref=stat_send.at[n],
                    dst_ref=stat_all.at[n, d],
                    send_sem=stat_send_sems.at[n],
                    recv_sem=stat_recv_sems.at[n],
                    device_id={"rows": row_at(d)},
                    device_id_type=MESH,
                ).start()

        def coef(self, d):
            n = self.n
            return pltpu.make_async_remote_copy(
                src_ref=coef_send.at[n],
                dst_ref=coef_all.at[n, d],
                send_sem=coef_send_sems.at[n, d],
                recv_sem=coef_recv_sems.at[n, d],
                device_id={"cols": lax.rem(k + d, num_cols)},
                device_id_type=MESH,
            )

        def settle(self):
            n = self.n
            everything = stat_all.at[n, pl.ds(1, num_rows - 1)]
            arrived = pltpu.make_async_remote_copy(
                src_ref=everything,
                dst_ref=everything,
                send_sem=stat_send_sems.at[n],
                recv_sem=stat_recv_sems.at[n],
                device_id={"rows": above},
                device_id_type=MESH,
            )
            arrived.wait_recv()
            pending.append(arrived)
            means = stat_all[n, :, 0, :]
            mean = jnp.sum(means, axis=0, keepdims=True) / num_rows
            spread = means - mean
            square = jnp.sum(stat_all[n, :, 1, :], axis=0, keepdims=True)
            square = square + count * jnp.sum(spread * spread, axis=0, keepdims=True)
            variance = square / (count * num_rows)
            scale = self.gain[...] / jnp.sqrt(variance + 1e-5)
            centres = [stat_all[n, d, 2:3, :] for d in (slot_above, 0, slot_below)]
            shifts = [(c - mean) * scale + self.bias[...] for c in centres]
            rows = jnp.concatenate([scale] + shifts, axis=0)
            coef_send[n] = rows
            coef_all[n, 0] = rows
            for d in range(1, num_cols):
                self.coef(d).start()

        def ready(self, q):
            for c in range(2):
                if q == 0 and c == 1:
                    continue
                owner = partner if q == 0 else at_chip(q) * 2 + c
                arrived = self.coef(lax.rem(k - owner + num_cols, num_cols))
                arrived.wait_recv()

        def sent(self):
            for d in range(1, num_cols):
                pending.append(self.coef(d))

    first = Gather(0, field_one, True)

    def look_up(i):
        unroll = 64

        def some(n, _):
            base = n * unroll
            line = i * parts + base // 128
            lane = lax.rem(base, 128)
            for u in range(unroll):
                row = ids_smem[line, lane + u]
                looked_ref[pl.ds(base + u, 1), :] = wide_ref[pl.ds(row, 1), :]
            return 0

        lax.fori_loop(0, width // unroll, some, 0)
        first.field[k, i + 1] = looked_ref[...].astype(BF16)

    look_up(0)
    pl.semaphore_wait(barrier, num_cols - 1 + 2)
    if rounds > 0:
        tell_known(0)

    def open_gather(gather):
        for i, j in ((0, 3), (1, 2), (3, 0)):
            gather.own_right(i)
            gather.own_left(j)
        for i in (0, 3, 1, 2):
            gather.own(i)

    def pass_first(gather):
        gather.from_left(0)
        gather.from_right(3)
        gather.own_right(2)
        gather.own_left(1)

    inner, outer, every = (1, 2), (0, 3), (0, 1, 2, 3)

    first.own_right(0)
    first.halo_out(0, k, 0)
    first.own(0)
    look_up(3)
    first.own_left(3)
    first.halo_out(0, k, 3)
    first.own(3)
    look_up(1)
    first.own_right(1)
    first.own(1)
    look_up(2)
    first.own_left(2)
    first.own(2)
    first.own_right(3)
    first.own_left(0)
    pass_first(first)
    first.halo_in(0)
    meet(0)
    first.from_left(1)
    first.from_right(2)
    lay_tokens()
    first.rest(0)
    late_loads[0].wait()
    convolve(field_one, True, conv_one_ref, 0, every, False)
    first.from_left(3)
    first.from_right(0)
    first.from_far(0)
    first.from_far(3)
    meet(1)
    first.from_left(2)
    first.from_right(1)
    first.halo_in(1)
    first.halo_in(2)
    first.rest_rows(1, every)
    convolve(field_one, True, conv_one_ref, 1, inner)
    first.from_far(1)
    first.from_far(2)
    first.rest_rows(2, every)
    convolve(field_one, True, conv_one_ref, 2, inner)
    first.halo_in(3)
    meet(2)
    first.rest_halo(1)
    convolve(field_one, True, conv_one_ref, 1, outer)
    first.rest_halo(2)
    convolve(field_one, True, conv_one_ref, 2, outer)
    first.rest_rows(3, every)
    convolve(field_one, True, conv_one_ref, 3, inner)
    first.rest_halo(3)
    convolve(field_one, True, conv_one_ref, 3, outer)

    second = Gather(1, field_two, True)
    norm_one = Norm(0, gain_one_ref, bias_one_ref)
    for i in (0, 3, 1, 2):
        norm_one.row(i, second)
    open_gather(second)
    meet(3)
    norm_one.tell()
    second.halo_out(0, k, 0)
    second.halo_out(0, k, 3)
    pass_first(second)
    second.halo_in(0)
    second.from_left(3)
    second.from_right(0)
    late_loads[3].wait()
    late_loads[4].wait()
    norm_one.settle()
    second.from_left(1)
    second.from_right(2)
    second.from_far(0)
    second.from_far(3)
    second.rest(0)
    late_loads[1].wait()
    norm_one.ready(0)
    slots = range(height + 2)
    normalise(second, 0, slots)
    convolve(hidden_ref, False, conv_two_ref, 0, every, False)
    second.from_left(2)
    second.from_right(1)
    second.halo_in(1)
    second.halo_in(2)
    second.from_far(1)
    second.from_far(2)
    middle, ends = range(1, height + 1), (0, height + 1)
    mine_only, other_only = (core,), (1 - core,)
    norm_one.ready(1)
    normalise(second, 1, middle, mine_only)
    norm_one.ready(2)
    normalise(second, 2, middle, mine_only)
    second.rest_rows(1, every)
    normalise(second, 1, middle, other_only)
    second.rest_rows(2, every)
    convolve(hidden_ref, False, conv_two_ref, 1, inner)
    normalise(second, 2, middle, other_only)
    second.halo_in(3)
    norm_one.ready(3)
    second.rest_halo(1)
    normalise(second, 1, ends)
    convolve(hidden_ref, False, conv_two_ref, 2, inner)
    normalise(second, 3, slots, mine_only)
    second.rest_halo(2)
    normalise(second, 2, ends)
    convolve(hidden_ref, False, conv_two_ref, 1, outer)
    second.rest(3)
    normalise(second, 3, slots, other_only)
    convolve(hidden_ref, False, conv_two_ref, 2, outer)
    convolve(hidden_ref, False, conv_two_ref, 3, every)
    norm_one.sent()

    third = Gather(2, field_three, False)
    norm_two = Norm(1, gain_two_ref, bias_two_ref)
    for i in (0, 3, 1, 2):
        norm_two.row(i, third)
    open_gather(third)
    norm_two.tell()
    pass_first(third)
    late_loads[5].wait()
    late_loads[6].wait()
    norm_two.settle()
    third.from_left(1)
    third.from_right(2)
    scale_two = coef_all[1, 0, 0:1, :]
    shift_two = coef_all[1, 0, 2:3, :]
    vocab_here = head_hbm.shape[1]
    tiles = vocab_here // 128

    def features_of(p, i):
        d = lax.rem(k - p + num_cols, num_cols)
        v = third.field[p, i].astype(F32) * coef_all[1, d, 0:1, :] + coef_all[1, d, 2:3, :]
        return (first.field[p, i + 1].astype(F32) + v).astype(BF16)

    def head_rows_of(q):
        at = at_chip(q)
        return head_ref[pl.ds(pl.multiple_of(at * 2 * lanes, 2 * lanes), 2 * lanes), :]

    def own_logits():
        for i in range(height):
            made = [features_of(at_chip(0) * 2 + c, i) for c in range(2)]
            early_ref[i] = jnp.dot(
                jnp.concatenate(made, axis=1), head_rows_of(0), preferred_element_type=F32
            )

    def all_features(i, to):
        for q in range(1, 4):
            for c in range(2):
                n = 2 * (q - 1) + c
                rows_ref[to, :, n * lanes : (n + 1) * lanes] = features_of(at_chip(q) * 2 + c, i)

    def row_logits(i, to):
        weights = jnp.concatenate([head_rows_of(q) for q in range(1, 4)], axis=0)
        logits_ref[to] = early_ref[i] + jnp.dot(
            rows_ref[to], weights, preferred_element_type=F32
        )

    def row_totals(i, to):
        most = logits_ref[to, :, 0:128]
        for t in range(1, tiles):
            most = jnp.maximum(most, logits_ref[to, :, 128 * t : 128 * t + 128])
        top = jnp.max(most, axis=1, keepdims=True)
        token = tokens_ref[i]
        lane = lax.broadcasted_iota(jnp.int32, (width, 128), 1)
        summed = jnp.zeros((width, 128), F32)
        picked = jnp.zeros((width, 128), F32)
        for t in range(tiles):
            part = logits_ref[to, :, 128 * t : 128 * t + 128]
            summed = summed + jnp.exp(part - top)
            ids = (lane + (k * vocab_here + 128 * t)).astype(F32)
            picked = picked + jnp.where(ids == token, part, 0.0)
        top_row = jnp.max(most.T, axis=0, keepdims=True)
        sum_row = jnp.sum(summed.T, axis=0, keepdims=True)
        pick_row = jnp.sum(picked.T, axis=0, keepdims=True)
        for n, row in enumerate((top_row, sum_row, pick_row)):
            for b in range(parts):
                last_send[b, n, i : i + 1, :] = row[:, 128 * b : 128 * b + 128]

    third.from_left(3)
    third.from_right(0)
    third.from_far(0)
    third.from_far(3)
    for i in range(height):
        v = conv_ref[i * width : (i + 1) * width, :] * scale_two + shift_two
        features_ref[i] = (first.field[k, i + 1].astype(F32) + v).astype(BF16)
    features_out = pltpu.make_async_copy(features_ref, features_hbm, load_sems.at[16])
    features_out.start()
    third.rest_rows(0, every)
    late_loads[2].wait()
    norm_two.ready(0)
    own_logits()
    third.from_left(2)
    third.from_right(1)
    for q in range(1, 4):
        third.rest_rows(q, (0, 3))
        norm_two.ready(q)
    norm_two.sent()
    all_features(0, 0)
    row_logits(0, 0)
    all_features(3, 1)
    third.from_far(1)
    third.from_far(2)
    row_logits(3, 1)
    row_totals(0, 0)
    for q in range(1, 4):
        third.rest_rows(q, (1, 2))
    all_features(1, 0)
    row_logits(1, 0)
    row_totals(3, 1)
    all_features(2, 1)
    row_logits(2, 1)
    row_totals(1, 0)
    row_totals(2, 1)

    per_block = num_cols // parts

    def exchange(d):
        to = lax.rem(k + d, num_cols)
        return pltpu.make_async_remote_copy(
            src_ref=last_send.at[to // per_block],
            dst_ref=last_all.at[d],
            send_sem=last_send_sems.at[d],
            recv_sem=last_recv_sems.at[d],
            device_id={"cols": to},
            device_id_type=MESH,
        )

    for d in range(1, num_cols):
        exchange(d).start()
    last_all[0] = last_send[k // per_block]
    for d in range(1, num_cols):
        exchange(d).wait_recv()
    totals_ref[...] = last_all[...]
    features_out.wait()

    for copy in pending:
        copy.wait_send()
    for d in range(1, num_cols):
        exchange(d).wait_send()


def finish(num_cols, made_ref, last_all, features_ref, logp_ref):
    features_ref[...] = made_ref[...]
    per_block = num_cols // (made_ref.shape[1] // 128)
    mine = made_ref.shape[1] // num_cols
    top = last_all[0, 0]
    for d in range(1, num_cols):
        top = jnp.maximum(top, last_all[d, 0])
    summed = jnp.zeros_like(top)
    picked = jnp.zeros_like(top)
    for d in range(num_cols):
        summed = summed + last_all[d, 1] * jnp.exp(last_all[d, 0] - top)
        picked = picked + last_all[d, 2]
    logp = picked - top - jnp.log(summed)
    place = lax.rem(lax.axis_index("cols"), per_block)
    out = logp[:, 0:mine]
    for b in range(1, per_block):
        out = jnp.where(place == b, logp[:, mine * b : mine * b + mine], out)
    logp_ref[...] = out


def local(
    token_ids,
    keep_mask,
    remask_order,
    embed_table,
    mask_embed,
    conv_one,
    gain_one,
    bias_one,
    conv_two,
    gain_two,
    bias_two,
    head_weight,
):
    num_rows, num_cols = lax.axis_size("rows"), lax.axis_size("cols")
    height, width = token_ids.shape
    vocab, lanes = embed_table.shape
    lines = height * width // 128
    in_vmem = pl.BlockSpec(memory_space=pltpu.VMEM)
    anywhere = pl.BlockSpec(memory_space=pl.ANY)
    made, totals = pl.pallas_call(
        functools.partial(kernel, num_rows, num_cols),
        name="denoise",
        out_shape=(
            jax.ShapeDtypeStruct((height, width, lanes), BF16),
            jax.ShapeDtypeStruct((num_cols, 3, height, 128), F32),
        ),
        in_specs=[anywhere] * 12,
        out_specs=(anywhere, in_vmem),
        scratch_shapes=[
            pltpu.VMEM((height, width), jnp.int32),
            pltpu.VMEM((height, width), jnp.int32),
            pltpu.VMEM((lines, 128), jnp.int32),
            pltpu.VMEM((1, lanes), BF16),
            pltpu.VMEM((1, lanes), F32),
            pltpu.VMEM((1, lanes), F32),
            pltpu.VMEM((1, lanes), F32),
            pltpu.VMEM((1, lanes), F32),
            pltpu.VMEM((height, width, lanes), BF16),
            pltpu.VMEM((vocab, lanes), BF16),
            pltpu.VMEM((vocab + 8, lanes), F32),
            pltpu.VMEM(conv_one.shape, BF16),
            pltpu.VMEM(conv_two.shape, BF16),
            pltpu.VMEM(head_weight.shape, BF16),
            pltpu.VMEM((lines, 128), jnp.int32),
            pltpu.SMEM((lines, 128), jnp.int32),
            pltpu.VMEM((height, width, 128), F32),
            pltpu.VMEM((width, lanes), F32),
            pltpu.VMEM((num_cols, height + 2, width, lanes), BF16),
            pltpu.VMEM((num_cols, height + 2, width, lanes), BF16),
            pltpu.VMEM((num_cols, height, width, lanes), BF16),
            pltpu.VMEM((height * width, 3 * lanes), F32),
            pltpu.VMEM((height * width, lanes), F32),
            pltpu.VMEM((2, 4, lanes), F32),
            pltpu.VMEM((2, num_rows, 4, lanes), F32),
            pltpu.VMEM((2, 4, lanes), F32),
            pltpu.VMEM((2, num_cols, 4, lanes), F32),
            pltpu.VMEM((num_cols, height + 2, width, lanes), BF16),
            pltpu.VMEM((2, width, (num_cols - 2) * lanes), BF16),
            pltpu.VMEM((height, width, head_weight.shape[1]), F32),
            pltpu.VMEM((2, width, head_weight.shape[1]), F32),
            pltpu.VMEM((width // 128, 3, height, 128), F32),
            pltpu.VMEM((num_cols, 3, height, 128), F32),
            pltpu.SemaphoreType.DMA((17,)),
            pltpu.SemaphoreType.DMA((3, 11, 4)),
            pltpu.SemaphoreType.DMA((3, 11, 4)),
            pltpu.SemaphoreType.DMA((2,)),
            pltpu.SemaphoreType.DMA((2,)),
            pltpu.SemaphoreType.DMA((2, num_cols)),
            pltpu.SemaphoreType.DMA((2, num_cols)),
            pltpu.SemaphoreType.DMA((num_cols,)),
            pltpu.SemaphoreType.DMA((num_cols,)),
            pltpu.SemaphoreType.REGULAR((8,)),
        ],
        compiler_params=pltpu.CompilerParams(
            collective_id=0, has_side_effects=True, vmem_limit_bytes=60 * 1024 * 1024
        ),
    )(
        token_ids,
        keep_mask,
        remask_order.reshape(lines, 128),
        embed_table,
        mask_embed.reshape(1, lanes),
        conv_one,
        gain_one.reshape(1, lanes),
        bias_one.reshape(1, lanes),
        conv_two,
        gain_two.reshape(1, lanes),
        bias_two.reshape(1, lanes),
        head_weight,
    )
    return pl.pallas_call(
        functools.partial(finish, num_cols),
        name="finish",
        out_shape=(
            jax.ShapeDtypeStruct((height, width, lanes), BF16),
            jax.ShapeDtypeStruct((height, width // num_cols), F32),
        ),
        in_specs=[in_vmem, in_vmem],
        out_specs=(in_vmem, in_vmem),
    )(made, totals)


def solution(mesh):
    in_specs = (
        P("rows", None),
        P("rows", None),
        P("rows"),
        P(None, "cols"),
        P("cols"),
        P(None, None, None, "cols"),
        P("cols"),
        P("cols"),
        P(None, None, None, "cols"),
        P("cols"),
        P("cols"),
        P(None, "cols"),
    )
    out_specs = (P("rows", None, "cols"), P("rows", "cols"))
    return jax.shard_map(local, mesh=mesh, in_specs=in_specs, out_specs=out_specs, check_vma=False)
```
